8 devices in a mesh: data: 4 (over z, y, x), stage: 2 (over core).
Axes of the slice: x: 2, y: 2, z: 1, core: 2. Of those that a mesh axis runs over, the one named last changes fastest.
Arguments:
- w_first: float32 [2, 512, 2048], P('stage')
- w_second: float32 [2, 2048, 512], P('stage')
- mom_first: float32 [2, 512, 2048], P('stage')
- mom_second: float32 [2, 2048, 512], P('stage')
- vel_first: float32 [2, 512, 2048], P('stage')
- vel_second: float32 [2, 2048, 512], P('stage')
- grad_first: float32 [2, 512, 2048], P('stage')
- grad_second: float32 [2, 2048, 512], P('stage')
- embed_table: float32 [32128, 512], replicated
- mom_embed: float32 [32128, 512], replicated
- vel_embed: float32 [32128, 512], replicated
- grad_embed: float32 [32128, 512], replicated
- stage_acts: bfloat16 [2, 4096, 512], P('stage', 'data')
- last_tokens: int32 [4096], P('data')
- targets: int32 [4096], P('data')
- next_tokens: int32 [16, 4096], P(None, 'data')
- max_norm: float32 [1], replicated
Outputs:
- output 1: float32 [2, 512, 2048], P('stage')
- output 2: float32 [2, 2048, 512], P('stage')
- output 3: float32 [2, 512, 2048], P('stage')
- output 4: float32 [2, 2048, 512], P('stage')
- output 5: float32 [2, 512, 2048], P('stage')
- output 6: float32 [2, 2048, 512], P('stage')
- output 7: float32 [32128, 512], replicated
- output 8: float32 [32128, 512], replicated
- output 9: float32 [32128, 512], replicated
- output 10: bfloat16 [16, 4096, 512], P(None, 'data')
All inputs are finite; a program needn't handle non-finite values.
Results may differ from the reference program's by a relative error of at most 0.00534546.
Values are sent between devices in bfloat16 or wider.
A program may use at most 2.25 GiB of HBM per device.

```python
import jax
import jax.numpy as jnp
from jax import lax

D = 512
FF = 2048
VOCAB = 32128
TOKENS = 1024
NEXT_MICRO = 16
STAGES = 2
REPLICAS = 4
STEP_COUNT = 10

EMB_SCALE = D ** 0.5
LEARN_RATE = 1e-3
ADAM_BETA1 = 0.9
ADAM_BETA2 = 0.95
ADAM_EPS = 1e-8
WEIGHT_DECAY = 0.1
CLIP_EPS = 1e-6


def setup_inputs(seed: int = 0) -> dict:
    rng_keys = jax.random.split(jax.random.key(seed), 17)
    n_rows = REPLICAS * TOKENS
    scale_first = 0.5 * (TOKENS / (FF * STAGES * REPLICAS)) ** 0.5
    scale_second = 0.5 * (TOKENS / (D * REPLICAS)) ** 0.5
    scale_embed = (TOKENS / (VOCAB * REPLICAS)) ** 0.5
    shape_first = (STAGES, D, FF)
    shape_second = (STAGES, FF, D)
    shape_embed = (VOCAB, D)
    w_first = jax.random.normal(rng_keys[0], shape_first, jnp.float32) * D ** -0.5
    w_second = jax.random.normal(rng_keys[1], shape_second, jnp.float32) * (FF * STAGES) ** -0.5
    embed_table = jax.random.normal(rng_keys[2], shape_embed, jnp.float32) * D ** -0.5
    grad_first = jax.random.normal(rng_keys[3], shape_first, jnp.float32) * scale_first
    grad_second = jax.random.normal(rng_keys[4], shape_second, jnp.float32) * scale_second
    grad_embed = jax.random.normal(rng_keys[5], shape_embed, jnp.float32) * scale_embed
    mom_first = jax.random.normal(rng_keys[6], shape_first, jnp.float32) * (0.4 * scale_first)
    mom_second = jax.random.normal(rng_keys[7], shape_second, jnp.float32) * (0.4 * scale_second)
    mom_embed = jax.random.normal(rng_keys[8], shape_embed, jnp.float32) * (0.4 * scale_embed)
    vel_first = jax.random.uniform(rng_keys[9], shape_first, jnp.float32, 0.25, 1.25) * (0.4 * scale_first) ** 2
    vel_second = jax.random.uniform(rng_keys[10], shape_second, jnp.float32, 0.25, 1.25) * (0.4 * scale_second) ** 2
    vel_embed = jax.random.uniform(rng_keys[11], shape_embed, jnp.float32, 0.25, 1.25) * (0.4 * scale_embed) ** 2
    stage_acts = jax.random.normal(rng_keys[12], (STAGES, n_rows, D), jnp.float32).astype(jnp.bfloat16)
    last_tokens = jax.random.randint(rng_keys[13], (n_rows,), 0, VOCAB, jnp.int32)
    targets = jax.random.randint(rng_keys[14], (n_rows,), 0, VOCAB, jnp.int32)
    next_tokens = jax.random.randint(rng_keys[15], (NEXT_MICRO, n_rows), 0, VOCAB, jnp.int32)
    grad_size = jnp.sqrt(jnp.sum(grad_first ** 2) + jnp.sum(grad_second ** 2) + jnp.sum(grad_embed ** 2))
    max_norm = grad_size * jax.random.uniform(rng_keys[16], (1,), jnp.float32, 0.5, 0.8)
    return {'w_first': w_first, 'w_second': w_second, 'mom_first': mom_first, 'mom_second': mom_second,
            'vel_first': vel_first, 'vel_second': vel_second, 'grad_first': grad_first, 'grad_second': grad_second,
            'embed_table': embed_table, 'mom_embed': mom_embed, 'vel_embed': vel_embed, 'grad_embed': grad_embed,
            'stage_acts': stage_acts, 'last_tokens': last_tokens, 'targets': targets, 'next_tokens': next_tokens,
            'max_norm': max_norm}


def block_forward(act_in, w_in, w_out):
    pre_act = jnp.dot(act_in, w_in, preferred_element_type=jnp.float32)
    hidden = jax.nn.gelu(pre_act).astype(jnp.bfloat16)
    mlp_out = jnp.dot(hidden, w_out, preferred_element_type=jnp.float32)
    return (act_in.astype(jnp.float32) + mlp_out).astype(jnp.bfloat16)


def block_backward(d_out, inputs):
    act_in, w_in, w_out = inputs
    pre_act = jnp.dot(act_in, w_in, preferred_element_type=jnp.float32)
    hidden, gelu_back = jax.vjp(jax.nn.gelu, pre_act)
    grad_out = jnp.dot(hidden.astype(jnp.bfloat16).T, d_out, preferred_element_type=jnp.float32)
    d_hidden = jnp.dot(d_out, w_out.T, preferred_element_type=jnp.float32)
    d_pre = gelu_back(d_hidden)[0].astype(jnp.bfloat16)
    grad_in = jnp.dot(act_in.T, d_pre, preferred_element_type=jnp.float32)
    d_act = (d_out.astype(jnp.float32) + jnp.dot(d_pre, w_in.T, preferred_element_type=jnp.float32)).astype(jnp.bfloat16)
    return d_act, (grad_in, grad_out)


def adamw_update(master, moment, velocity, gradient, clip_scale):
    scaled_grad = clip_scale * gradient
    moment_new = ADAM_BETA1 * moment + (1.0 - ADAM_BETA1) * scaled_grad
    velocity_new = ADAM_BETA2 * velocity + (1.0 - ADAM_BETA2) * scaled_grad * scaled_grad
    moment_hat = moment_new / (1.0 - ADAM_BETA1 ** STEP_COUNT)
    velocity_hat = velocity_new / (1.0 - ADAM_BETA2 ** STEP_COUNT)
    master_new = master - LEARN_RATE * (moment_hat / (jnp.sqrt(velocity_hat) + ADAM_EPS) + WEIGHT_DECAY * master)
    return master_new, moment_new, velocity_new


def reference(w_first, w_second, mom_first, mom_second, vel_first, vel_second, grad_first, grad_second,
              embed_table, mom_embed, vel_embed, grad_embed, stage_acts, last_tokens, targets, next_tokens, max_norm):
    first_b = w_first.astype(jnp.bfloat16)
    second_b = w_second.astype(jnp.bfloat16)
    table_b = embed_table.astype(jnp.bfloat16)
    vocab_ids = jnp.arange(VOCAB)

    def replica_step(grad_sums, inputs):
        acts_rep, tok_rep, tgt_rep = inputs
        top_out = block_forward(acts_rep[STAGES - 1], first_b[STAGES - 1], second_b[STAGES - 1])
        logits = jnp.dot(top_out, table_b.T, preferred_element_type=jnp.float32)
        soft_probs = jax.nn.softmax(logits, axis=-1)
        d_logits = jnp.where(vocab_ids[None, :] == tgt_rep[:, None], soft_probs - 1.0, soft_probs).astype(jnp.bfloat16)
        d_top = jnp.dot(d_logits, table_b, preferred_element_type=jnp.float32).astype(jnp.bfloat16)
        head_grad = jnp.dot(d_logits.T, top_out, preferred_element_type=jnp.float32)
        d_low, (grads_in, grads_out) = lax.scan(block_backward, d_top, (acts_rep, first_b, second_b), reverse=True)
        low_grad = EMB_SCALE * jax.ops.segment_sum(d_low.astype(jnp.float32), tok_rep, num_segments=VOCAB)
        sum_first, sum_second, sum_embed = grad_sums
        return (sum_first + grads_in, sum_second + grads_out, sum_embed + head_grad + low_grad), None

    per_replica = (jnp.transpose(stage_acts.reshape(STAGES, REPLICAS, TOKENS, D), (1, 0, 2, 3)),
                   last_tokens.reshape(REPLICAS, TOKENS), targets.reshape(REPLICAS, TOKENS))
    zero_init = (jnp.zeros_like(w_first), jnp.zeros_like(w_second), jnp.zeros_like(embed_table))
    (sum_first, sum_second, sum_embed), _ = lax.scan(replica_step, zero_init, per_replica)
    full_first = grad_first + sum_first / REPLICAS
    full_second = grad_second + sum_second / REPLICAS
    full_embed = grad_embed + sum_embed / REPLICAS
    total_sq = jnp.sum(full_first ** 2) + jnp.sum(full_second ** 2) + jnp.sum(full_embed ** 2)
    clip_scale = jnp.minimum(1.0, max_norm[0] / (jnp.sqrt(total_sq) + CLIP_EPS))
    new_first, new_mom_first, new_vel_first = adamw_update(w_first, mom_first, vel_first, full_first, clip_scale)
    new_second, new_mom_second, new_vel_second = adamw_update(w_second, mom_second, vel_second, full_second, clip_scale)
    new_embed, new_mom_embed, new_vel_embed = adamw_update(embed_table, mom_embed, vel_embed, full_embed, clip_scale)
    next_first_b = new_first.astype(jnp.bfloat16)
    next_second_b = new_second.astype(jnp.bfloat16)
    next_table_b = new_embed.astype(jnp.bfloat16)

    def run_rows(tok_row):
        start_act = (EMB_SCALE * jnp.take(next_table_b, tok_row, axis=0).astype(jnp.float32)).astype(jnp.bfloat16)

        def layer_step(carry_act, weights):
            return block_forward(carry_act, weights[0], weights[1]), None

        out_act, _ = lax.scan(layer_step, start_act, (next_first_b, next_second_b))
        return out_act

    next_acts = lax.map(run_rows, next_tokens.reshape(NEXT_MICRO * REPLICAS, TOKENS)).reshape(NEXT_MICRO, REPLICAS * TOKENS, D)
    return (new_first, new_second, new_mom_first, new_mom_second, new_vel_first, new_vel_second,
            new_embed, new_mom_embed, new_vel_embed, next_acts)
```

```python
import functools
import math
import jax
import jax.numpy as jnp
from jax import lax
from jax.experimental import pallas as pl
from jax.experimental.pallas import tpu as pltpu
from jax.sharding import PartitionSpec as P

STEP_COUNT = 10
LEARN_RATE = 1e-3
ADAM_BETA1 = 0.9
ADAM_BETA2 = 0.95
ADAM_EPS = 1e-8
WEIGHT_DECAY = 0.1
CLIP_EPS = 1e-6

TILE = 512
ADAM_TILE = 1024
CHUNK = 512
SEG = 128
TOKEN_BLOCK = 512
FF_CHUNK = 512
WIDE_TILES = 5
NEG = -1e30
GELU_K = math.sqrt(2.0 / math.pi)
GELU_A = 0.044715
BOTH = ('data', 'stage')


def block_forward(act_in, w_in, w_out):
    pre_act = jnp.dot(act_in, w_in, preferred_element_type=jnp.float32)
    hidden = jax.nn.gelu(pre_act).astype(jnp.bfloat16)
    mlp_out = jnp.dot(hidden, w_out, preferred_element_type=jnp.float32)
    return (act_in.astype(jnp.float32) + mlp_out).astype(jnp.bfloat16)


def backward_kernel(n_chunks, g_ref, x_ref, wi_ref, wo_ref, dx_ref, dwi_ref, dwo_ref, back_ref, acc_i, acc_o):
    f = pl.program_id(0)
    wi = wi_ref[...]
    wi_flip = wi.T
    acc_i[...] = jnp.zeros_like(acc_i)
    acc_o[...] = jnp.zeros_like(acc_o)

    @pl.when(f == 0)
    def _():
        back_ref[...] = jnp.zeros_like(back_ref)

    def chunk(c, _):
        rows = pl.ds(pl.multiple_of(c * CHUNK, CHUNK), CHUNK)
        x, g = x_ref[rows, :], g_ref[rows, :]
        pre = dot_last(wi_flip, x)
        d_hidden = dot_last(wo_ref[...], g)
        square = pre * pre
        bend = jnp.tanh(GELU_K * pre * (1.0 + GELU_A * square))
        rise = 0.5 * (1.0 + bend)
        hidden = (pre * rise).astype(jnp.bfloat16)
        slope = rise + (0.5 * GELU_K) * pre * (1.0 - bend * bend) * (1.0 + (3.0 * GELU_A) * square)
        d_pre = (d_hidden * slope).astype(jnp.bfloat16)
        acc_o[...] += jnp.dot(hidden, g, preferred_element_type=jnp.float32)
        acc_i[...] += jnp.dot(d_pre, x, preferred_element_type=jnp.float32)
        back_ref[c] += jnp.dot(wi, d_pre, preferred_element_type=jnp.float32)
        return 0

    lax.fori_loop(0, n_chunks, chunk, 0, unroll=2)
    dwo_ref[...] = acc_o[...]
    dwi_ref[...] = acc_i[...].T

    @pl.when(f == pl.num_programs(0) - 1)
    def _():
        def last(c, _):
            rows = pl.ds(pl.multiple_of(c * CHUNK, CHUNK), CHUNK)
            dx_ref[rows, :] = (g_ref[rows, :].astype(jnp.float32) + back_ref[c].T).astype(jnp.bfloat16)
            return 0
        lax.fori_loop(0, n_chunks, last, 0)


def block_backward(d_out, act_in, w_in, w_out):
    n_tok, d_model = act_in.shape
    ff = w_in.shape[1]
    n_chunks = n_tok // CHUNK
    tokens = pl.BlockSpec((n_tok, d_model), lambda f: (0, 0))
    cols = pl.BlockSpec((d_model, FF_CHUNK), lambda f: (0, f))
    rows = pl.BlockSpec((FF_CHUNK, d_model), lambda f: (f, 0))
    return pl.pallas_call(
        functools.partial(backward_kernel, n_chunks),
        out_shape=[jax.ShapeDtypeStruct((n_tok, d_model), jnp.bfloat16), jax.ShapeDtypeStruct((d_model, ff), jnp.float32),
                   jax.ShapeDtypeStruct((ff, d_model), jnp.float32)],
        grid=(ff // FF_CHUNK,),
        in_specs=[tokens, tokens, cols, rows],
        out_specs=[tokens, cols, rows],
        scratch_shapes=[pltpu.VMEM((n_chunks, d_model, CHUNK), jnp.float32), pltpu.VMEM((FF_CHUNK, d_model), jnp.float32),
                        pltpu.VMEM((FF_CHUNK, d_model), jnp.float32)],
        compiler_params=params(),
        cost_estimate=pl.CostEstimate(flops=10 * n_tok * d_model * ff, bytes_accessed=12 * d_model * ff, transcendentals=0),
        name='block_backward',
    )(d_out, act_in, w_in, w_out)


def adamw_update(master, moment, velocity, gradient, clip_scale):
    scaled_grad = clip_scale * gradient
    moment_new = ADAM_BETA1 * moment + (1.0 - ADAM_BETA1) * scaled_grad
    velocity_new = ADAM_BETA2 * velocity + (1.0 - ADAM_BETA2) * scaled_grad * scaled_grad
    moment_hat = moment_new / (1.0 - ADAM_BETA1 ** STEP_COUNT)
    velocity_hat = velocity_new / (1.0 - ADAM_BETA2 ** STEP_COUNT)
    master_new = master - LEARN_RATE * (moment_hat / (jnp.sqrt(velocity_hat) + ADAM_EPS) + WEIGHT_DECAY * master)
    return master_new, moment_new, velocity_new


def dot_last(a, b):
    return lax.dot_general(a, b, (((1,), (1,)), ((), ())), preferred_element_type=jnp.float32)


def params(limit_mib=60, **kw):
    return pltpu.CompilerParams(vmem_limit_bytes=limit_mib * 1024 * 1024, **kw)


def load_rows(block, e_ref, vocab):
    rows = block * TILE + lax.broadcasted_iota(jnp.int32, (TILE, 1), 0)
    valid = rows < vocab
    e_tile = jnp.where(valid, e_ref[...], 0.0).astype(jnp.bfloat16)
    return rows, valid, e_tile, jnp.where(valid, 0.0, NEG)


def tile_of(n_own, blk_ref, j):
    return jnp.where(j < n_own, blk_ref[0] + j, blk_ref[1] + j)


def stats_kernel(vocab, n_chunks, n_own, blk_ref, z_ref, e_ref, stat_ref):
    _, _, e_tile, bias = load_rows(tile_of(n_own, blk_ref, pl.program_id(0)), e_ref, vocab)

    @pl.when(pl.program_id(0) == 0)
    def _():
        stat_ref[0:1, :] = jnp.full((1, stat_ref.shape[1]), NEG, jnp.float32)
        stat_ref[1:2, :] = jnp.zeros((1, stat_ref.shape[1]), jnp.float32)

    def chunk(c, _):
        cols = pl.ds(pl.multiple_of(c * CHUNK, CHUNK), CHUNK)
        logits = dot_last(e_tile, z_ref[cols, :]) + bias
        top_old = stat_ref[0:1, cols]
        top_new = jnp.maximum(top_old, jnp.max(logits, axis=0, keepdims=True))
        part = jnp.sum(jnp.exp(logits - top_new), axis=0, keepdims=True)
        stat_ref[0:1, cols] = top_new
        stat_ref[1:2, cols] = stat_ref[1:2, cols] * jnp.exp(top_old - top_new) + part
        return 0

    lax.fori_loop(0, n_chunks, chunk, 0, unroll=4)


def head_stats(z_all, embed_table, blocks, n_own, n_tiles):
    vocab, d_model = embed_table.shape
    n_tok = z_all.shape[0]
    last = (vocab - 1) // TILE
    return pl.pallas_call(
        functools.partial(stats_kernel, vocab, n_tok // CHUNK, n_own),
        out_shape=jax.ShapeDtypeStruct((2, n_tok), jnp.float32),
        grid_spec=pltpu.PrefetchScalarGridSpec(
            num_scalar_prefetch=1, grid=(n_tiles,),
            in_specs=[pl.BlockSpec((n_tok, d_model), lambda j, b: (0, 0)),
                      pl.BlockSpec((TILE, d_model), lambda j, b: (jnp.minimum(tile_of(n_own, b, j), last), 0))],
            out_specs=pl.BlockSpec((2, n_tok), lambda j, b: (0, 0))),
        compiler_params=params(),
        cost_estimate=pl.CostEstimate(flops=2 * n_tiles * TILE * n_tok * d_model, bytes_accessed=n_tiles * TILE * d_model * 4, transcendentals=0),
        name='head_stats',
    )(blocks, z_all, embed_table)


def head_kernel(vocab, n_chunks, n_rep, n_own, with_top, blk_ref, z_ref, norm_ref, tgt_ref, e_ref, g_ref, out_ref, *rest):
    top_ref = rest[0] if with_top else None
    acc_ref = rest[-1]
    j = pl.program_id(0)
    rows, valid, e_tile, bias = load_rows(tile_of(n_own, blk_ref, j), e_ref, vocab)
    if with_top:
        e_flip = e_tile.T

        @pl.when(j == 0)
        def _():
            top_ref[...] = jnp.zeros_like(top_ref)

    def chunk(with_rows, c, _):
        cols = pl.ds(pl.multiple_of(c * CHUNK, CHUNK), CHUNK)
        z_chunk = z_ref[cols, :]
        logits = dot_last(e_tile, z_chunk) + bias
        probs = jnp.exp(logits - norm_ref[0:1, cols]) * norm_ref[1:2, cols]
        d_logits = jnp.where(rows == tgt_ref[0:1, cols], probs - 1.0, probs).astype(jnp.bfloat16)
        if with_rows:
            acc_ref[...] += jnp.dot(d_logits, z_chunk, preferred_element_type=jnp.float32)
        if with_top:
            top_ref[c] += jnp.dot(e_flip, d_logits, preferred_element_type=jnp.float32)
        return 0

    @pl.when(j < n_own)
    def _():
        acc_ref[...] = jnp.zeros_like(acc_ref)
        lax.fori_loop(0, n_chunks, functools.partial(chunk, True), 0, unroll=2 if with_top else 4)
        out_ref[...] = jnp.where(valid, g_ref[...], 0.0) + acc_ref[...] * (1.0 / n_rep)

    if with_top:
        @pl.when(j >= n_own)
        def _():
            lax.fori_loop(0, n_chunks, functools.partial(chunk, False), 0, unroll=2)


def head_grads(z_all, norm, targets, embed_table, grad_embed, blocks, n_own, n_tiles, n_rep, with_top):
    vocab, d_model = embed_table.shape
    n_tok = z_all.shape[0]
    n_chunks = n_tok // CHUNK
    last = (vocab - 1) // TILE
    out_shape = [jax.ShapeDtypeStruct((n_own * TILE, d_model), jnp.float32)]
    out_specs = [pl.BlockSpec((TILE, d_model), lambda j, b: (jnp.minimum(j, n_own - 1), 0))]
    if with_top:
        out_shape.append(jax.ShapeDtypeStruct((n_chunks, d_model, CHUNK), jnp.float32))
        out_specs.append(pl.BlockSpec((n_chunks, d_model, CHUNK), lambda j, b: (0, 0, 0)))
    return pl.pallas_call(
        functools.partial(head_kernel, vocab, n_chunks, n_rep, n_own, with_top),
        out_shape=out_shape,
        grid_spec=pltpu.PrefetchScalarGridSpec(
            num_scalar_prefetch=1, grid=(n_tiles,),
            in_specs=[pl.BlockSpec((n_tok, d_model), lambda j, b: (0, 0)),
                      pl.BlockSpec((2, n_tok), lambda j, b: (0, 0)),
                      pl.BlockSpec((1, n_tok), lambda j, b: (0, 0)),
                      pl.BlockSpec((TILE, d_model), lambda j, b: (jnp.minimum(tile_of(n_own, b, j), last), 0)),
                      pl.BlockSpec((TILE, d_model), lambda j, b: (jnp.minimum(b[0] + jnp.minimum(j, n_own - 1), last), 0))],
            out_specs=out_specs,
            scratch_shapes=[pltpu.VMEM((TILE, d_model), jnp.float32)]),
        compiler_params=params(),
        cost_estimate=pl.CostEstimate(flops=(6 if with_top else 4) * n_tiles * TILE * n_tok * d_model,
                                      bytes_accessed=n_tiles * TILE * d_model * 12, transcendentals=0),
        name='head_grads' if with_top else 'head_rows',
    )(blocks, z_all, norm, targets, embed_table, grad_embed)


def sparse_rows(block, start_ref, ids_ref, low_ref, base):
    rows = block * TILE + lax.broadcasted_iota(jnp.int32, (TILE, 1), 0)
    first = start_ref[block] // SEG
    stop = (start_ref[block + 1] + SEG - 1) // SEG

    def segment(c, acc):
        pick = jnp.where(rows == ids_ref[pl.ds(c, 1), :], 1.0, 0.0).astype(jnp.bfloat16)
        return acc + jnp.dot(pick, low_ref[pl.ds(pl.multiple_of(c * SEG, SEG), SEG), :], preferred_element_type=jnp.float32)

    return lax.fori_loop(first, stop, segment, base)


def sumsq_kernel(low_scale, blk_ref, start_ref, ids_ref, low_ref, g_ref, out_ref):
    block = blk_ref[0] + pl.program_id(0)
    zero = jnp.zeros(g_ref.shape, jnp.float32)
    full = g_ref[...] + low_scale * sparse_rows(block, start_ref, ids_ref, low_ref, zero)

    @pl.when(pl.program_id(0) == 0)
    def _():
        out_ref[...] = jnp.zeros_like(out_ref)

    out_ref[...] += jnp.sum((full * full).reshape(-1, 8, full.shape[1]), axis=0)


def rows_sumsq(blocks, starts, ids, low, g_rows, n_tiles, low_scale):
    d_model = g_rows.shape[1]
    return pl.pallas_call(
        functools.partial(sumsq_kernel, low_scale),
        out_shape=jax.ShapeDtypeStruct((8, d_model), jnp.float32),
        grid_spec=pltpu.PrefetchScalarGridSpec(
            num_scalar_prefetch=2, grid=(n_tiles,),
            in_specs=[pl.BlockSpec(ids.shape, lambda j, b, s: (0, 0)),
                      pl.BlockSpec(low.shape, lambda j, b, s: (0, 0)),
                      pl.BlockSpec((TILE, d_model), lambda j, b, s: (b[1] + j, 0))],
            out_specs=pl.BlockSpec((8, d_model), lambda j, b, s: (0, 0))),
        compiler_params=params(),
        name='rows_sumsq',
    )(blocks, starts, ids, low, g_rows)


def adam_kernel(low_scale, n_wide, n_red, start_ref, stage_ref, clip_ref, ids_ref, low_ref, gw_ref, go_ref, gf_ref,
                w_ref, m_ref, v_ref, w_out, m_out, v_out, acc_ref):
    j = pl.program_id(0)
    own = n_wide + n_red * stage_ref[0]
    is_own = (j >= own) & (j < own + n_red)

    @pl.when(j < n_wide)
    def _():
        acc_ref[...] = gw_ref[...]

    @pl.when(is_own)
    def _():
        acc_ref[...] = go_ref[...]

    @pl.when((j >= n_wide) & jnp.logical_not(is_own))
    def _():
        acc_ref[...] = gf_ref[...]

    rows = j * ADAM_TILE + lax.broadcasted_iota(jnp.int32, (ADAM_TILE, 1), 0)

    def segment(c, _):
        pick = jnp.where(rows == ids_ref[pl.ds(c, 1), :], 1.0, 0.0).astype(jnp.bfloat16)
        acc_ref[...] += low_scale * jnp.dot(pick, low_ref[pl.ds(pl.multiple_of(c * SEG, SEG), SEG), :], preferred_element_type=jnp.float32)
        return 0

    per = ADAM_TILE // TILE
    lax.fori_loop(start_ref[per * j] // SEG, (start_ref[per * j + per] + SEG - 1) // SEG, segment, 0)

    def part(i, _):
        r = pl.ds(pl.multiple_of(i * 32, 32), 32)
        w_new, m_new, v_new = adamw_update(w_ref[r, :], m_ref[r, :], v_ref[r, :], acc_ref[r, :], clip_ref[0])
        w_out[r, :] = w_new
        m_out[r, :] = m_new
        v_out[r, :] = v_new
        return 0

    lax.fori_loop(0, ADAM_TILE // 32, part, 0)


def embed_adam(starts, stage, clip, ids, low, g_wide, g_own, g_far, embed_table, mom, vel, low_scale):
    vocab, d_model = embed_table.shape
    n_wide, n_red = g_wide.shape[0] // ADAM_TILE, g_own.shape[0] // ADAM_TILE
    spec = pl.BlockSpec((ADAM_TILE, d_model), lambda j, s, t, c: (j, 0))
    shape = jax.ShapeDtypeStruct((vocab, d_model), jnp.float32)

    def held(first):
        return pl.BlockSpec((ADAM_TILE, d_model), lambda j, s, t, c: (jnp.clip(j - n_wide - n_red * first(t[0]), 0, n_red - 1), 0))

    return pl.pallas_call(
        functools.partial(adam_kernel, low_scale, n_wide, n_red),
        out_shape=[shape] * 3,
        grid_spec=pltpu.PrefetchScalarGridSpec(
            num_scalar_prefetch=3, grid=(pl.cdiv(vocab, ADAM_TILE),),
            in_specs=[pl.BlockSpec(ids.shape, lambda j, s, t, c: (0, 0)),
                      pl.BlockSpec(low.shape, lambda j, s, t, c: (0, 0)),
                      pl.BlockSpec((ADAM_TILE, d_model), lambda j, s, t, c: (jnp.minimum(j, n_wide - 1), 0)),
                      held(lambda t: t), held(lambda t: 1 - t), spec, spec, spec],
            out_specs=[spec] * 3,
            scratch_shapes=[pltpu.VMEM((ADAM_TILE, d_model), jnp.float32)]),
        compiler_params=params(),
        cost_estimate=pl.CostEstimate(flops=20 * vocab * d_model, bytes_accessed=28 * vocab * d_model, transcendentals=0),
        name='embed_adam',
    )(starts, stage, clip, ids, low, g_wide, g_own, g_far, embed_table, mom, vel)


def next_kernel(scale, n_blocks, ids_ref, table_ref, wi0_ref, wo0_ref, wi1_ref, wo1_ref, out_ref, rows_ref, x_ref, acc_ref, sems):
    blk = pl.program_id(0)
    slot = lax.rem(blk, 2)
    n_ff = wi0_ref.shape[1] // FF_CHUNK
    per = TOKEN_BLOCK // (2 * n_ff)

    def fetch(base, to_slot, first, count):
        for t in range(count):
            row = ids_ref[base + first + t]
            pltpu.make_async_copy(table_ref.at[pl.ds(row, 1), :], rows_ref.at[to_slot, pl.ds(first + t, 1), :], sems.at[to_slot]).start()

    @pl.when(blk == 0)
    def _():
        def step(i, _):
            fetch(0, 0, i * 16, 16)
            return 0
        lax.fori_loop(0, TOKEN_BLOCK // 16, step, 0)

    pltpu.make_async_copy(rows_ref.at[1 - slot], rows_ref.at[slot], sems.at[slot]).wait()
    base = jnp.minimum(blk + 1, n_blocks - 1) * TOKEN_BLOCK
    more = blk + 1 < n_blocks
    x_ref[...] = (scale * rows_ref[slot].astype(jnp.bfloat16).astype(jnp.float32)).astype(jnp.bfloat16)

    for layer, (wi_ref, wo_ref) in enumerate(((wi0_ref, wo0_ref), (wi1_ref, wo1_ref))):
        acc_ref[...] = x_ref[...].astype(jnp.float32)
        for c in range(n_ff):
            @pl.when(more)
            def _():
                fetch(base, 1 - slot, (layer * n_ff + c) * per, per)
            cols = pl.ds(c * FF_CHUNK, FF_CHUNK)
            pre_act = jnp.dot(x_ref[...], wi_ref[:, cols], preferred_element_type=jnp.float32)
            hidden = jax.nn.gelu(pre_act).astype(jnp.bfloat16)
            acc_ref[...] += jnp.dot(hidden, wo_ref[cols, :], preferred_element_type=jnp.float32)
        if layer == 0:
            x_ref[...] = acc_ref[...].astype(jnp.bfloat16)
        else:
            out_ref[...] = acc_ref[...].astype(jnp.bfloat16)


def next_forward(ids, table, wi0, wo0, wi1, wo1, scale):
    n_tok = ids.shape[0]
    d_model = table.shape[1]
    whole = [pl.BlockSpec(w.shape, lambda j, s: (0, 0)) for w in (wi0, wo0, wi1, wo1)]
    return pl.pallas_call(
        functools.partial(next_kernel, scale, n_tok // TOKEN_BLOCK),
        out_shape=jax.ShapeDtypeStruct((n_tok, d_model), jnp.bfloat16),
        grid_spec=pltpu.PrefetchScalarGridSpec(
            num_scalar_prefetch=1, grid=(n_tok // TOKEN_BLOCK,),
            in_specs=[pl.BlockSpec(memory_space=pl.ANY)] + whole,
            out_specs=pl.BlockSpec((TOKEN_BLOCK, d_model), lambda j, s: (j, 0)),
            scratch_shapes=[pltpu.VMEM((2, TOKEN_BLOCK, d_model), jnp.float32), pltpu.VMEM((TOKEN_BLOCK, d_model), jnp.bfloat16),
                            pltpu.VMEM((TOKEN_BLOCK, d_model), jnp.float32), pltpu.SemaphoreType.DMA((2,))]),
        compiler_params=params(),
        cost_estimate=pl.CostEstimate(flops=8 * n_tok * d_model * wi0.shape[1], bytes_accessed=6 * n_tok * d_model, transcendentals=0),
        name='next_forward',
    )(ids, table, wi0, wo0, wi1, wo1)


def solution(mesh):
    n_stage = mesh.shape['stage']
    n_rep = mesh.shape['data']
    n_dev = n_stage * n_rep
    swap = [(0, 1), (1, 0)]
    w_spec = P('stage', None, None)
    in_specs = (w_spec,) * 8 + (P(None, None),) * 4 + (P('stage', 'data', None), P('data'), P('data'), P(None, 'data'), P(None))
    out_specs = (w_spec,) * 6 + (P(None, None),) * 3 + (P(None, 'data', None),)

    def local_step(w_first, w_second, mom_first, mom_second, vel_first, vel_second, grad_first, grad_second,
                   embed_table, mom_embed, vel_embed, grad_embed, stage_acts, last_tokens, targets, next_tokens, max_norm):
        stage_id = lax.axis_index('stage')
        dev_id = lax.axis_index('data') * n_stage + stage_id
        low_core = stage_id == 0
        vocab, d_model = embed_table.shape
        scale_in = math.sqrt(d_model)
        low_scale = scale_in / n_rep
        n_tiles = -(-vocab // (TILE * n_dev))
        n_wide = WIDE_TILES
        n_rest = n_tiles - n_wide
        n_red = n_rest * n_dev // n_stage
        n_part = n_red // n_rep
        rest0 = n_dev * n_wide

        def other(x):
            return lax.ppermute(x, 'stage', swap)

        def by_stage(own, far):
            return jnp.where(low_core, own, far), jnp.where(low_core, far, own)

        w_in, w_out = w_first[0].astype(jnp.bfloat16), w_second[0].astype(jnp.bfloat16)
        w_in0, w_in1 = by_stage(w_in, other(w_in))
        w_out0, w_out1 = by_stage(w_out, other(w_out))

        z_own = block_forward(stage_acts[0], w_in, w_out)
        cut = z_own.shape[0] // 2
        z_piece = jnp.where(low_core, lax.ppermute(z_own[:cut], 'stage', [(1, 0)]), z_own[cut:])
        all_ids = lax.all_gather(jnp.stack([last_tokens, targets]), 'data', axis=1, tiled=True)
        ids, tgts = all_ids[0], all_ids[1:2]
        n_tok = ids.shape[0]
        half = n_tok // 2
        z_all = lax.all_gather(z_piece, BOTH, axis=0, tiled=True)

        order = jnp.arange(n_tok, dtype=jnp.int32)
        before = (ids[None, :] < ids[:, None]) | ((ids[None, :] == ids[:, None]) & (order[None, :] < order[:, None]))
        rank = jnp.sum(before.astype(jnp.int32), axis=1)
        sorted_ids = jnp.sum(jnp.where(rank[None, :] == order[:, None], ids[None, :], 0), axis=1).reshape(n_tok // SEG, SEG)
        edges = TILE * jnp.arange(n_tiles * n_dev + 1, dtype=jnp.int32)
        starts = jnp.sum((ids[None, :] < edges[:, None]).astype(jnp.int32), axis=1)
        z_all, rank, sorted_ids, starts, acts_in = lax.optimization_barrier((z_all, rank, sorted_ids, starts, stage_acts[0]))

        acts = lax.all_gather(acts_in, 'data', axis=0, tiled=True)
        mine = lax.dynamic_slice_in_dim(acts, stage_id * half, half)
        far = other(lax.dynamic_slice_in_dim(acts, (1 - stage_id) * half, half))
        act0, act1 = by_stage(mine, far)

        def blocks(*tiles):
            return jnp.stack([jnp.asarray(t, jnp.int32) for t in tiles])

        shard = blocks(dev_id * n_wide, rest0 + dev_id * n_rest - n_wide)
        stat = head_stats(z_all, embed_table, shard, n_wide, n_tiles)
        stats = lax.all_gather(stat, BOTH, axis=0, tiled=False)
        top = jnp.max(stats[:, 0], axis=0)
        total = jnp.sum(stats[:, 1] * jnp.exp(stats[:, 0] - top[None]), axis=0)
        norm = jnp.stack([top, 1.0 / total])
        g_shard, d_top_part = head_grads(z_all, norm, tgts, embed_table, grad_embed, shard, n_wide, n_tiles, n_rep, True)
        d_top_part, act0, act1 = lax.optimization_barrier((d_top_part, act0, act1))
        d_top_own = lax.psum_scatter(d_top_part, BOTH, scatter_dimension=0, tiled=True)
        red_tile = rest0 + stage_id * n_red
        g_own = head_grads(z_all, norm, tgts, embed_table, grad_embed, blocks(red_tile, red_tile), n_red, n_red, n_rep, False)[0]
        d_top_own, g_own = lax.optimization_barrier((d_top_own, g_own))
        d_top_own = d_top_own.reshape(d_model, -1).T.astype(jnp.bfloat16)
        d_top = lax.all_gather(d_top_own, BOTH, axis=0, tiled=True)
        g_shard, d_top_own = lax.optimization_barrier((g_shard, d_top_own))
        g_far = other(g_own)
        g_wide = lax.all_gather(g_shard, BOTH, axis=0, tiled=True)

        d_half = lax.dynamic_slice_in_dim(d_top, stage_id * half, half)
        d_act1, g_in1, g_out1 = block_backward(d_half, act1, w_in1, w_out1)
        d_low_half, g_in0, g_out0 = block_backward(d_act1, act0, w_in0, w_out0)
        my_rank = lax.dynamic_slice_in_dim(rank, stage_id * half, half)
        perm = (my_rank[None, :] == order[:, None]).astype(jnp.bfloat16)
        low_half = jnp.dot(perm, d_low_half, preferred_element_type=jnp.float32).astype(jnp.bfloat16)
        low = low_half + other(low_half)

        def both_halves(part0, part1):
            far0, far1 = lax.ppermute(part0, 'stage', [(1, 0)]), lax.ppermute(part1, 'stage', [(0, 1)])
            return jnp.where(low_core, part0 + far0, part1 + far1)

        full_first = grad_first[0] + both_halves(g_in0, g_in1) / n_rep
        full_second = grad_second[0] + both_halves(g_out0, g_out1) / n_rep
        my_part = lax.axis_index('data') * n_part
        embed_sq = (jnp.sum(rows_sumsq(blocks(dev_id * n_wide, 0), starts, sorted_ids, low, g_shard, n_wide, low_scale))
                    + jnp.sum(rows_sumsq(blocks(red_tile + my_part, my_part), starts, sorted_ids, low, g_own, n_part, low_scale)))
        stage_sq = jnp.sum(full_first * full_first) + jnp.sum(full_second * full_second)
        parts_sq = lax.all_gather(jnp.full((1, 128), embed_sq + stage_sq / n_rep), BOTH, axis=0, tiled=True)
        total_sq = jnp.sum(parts_sq[:, 0])
        clip_scale = jnp.minimum(1.0, max_norm[0] / (jnp.sqrt(total_sq) + CLIP_EPS))
        new_first, new_mom_first, new_vel_first = adamw_update(w_first[0], mom_first[0], vel_first[0], full_first, clip_scale)
        new_second, new_mom_second, new_vel_second = adamw_update(w_second[0], mom_second[0], vel_second[0], full_second, clip_scale)
        new_embed, new_mom_embed, new_vel_embed = embed_adam(
            starts, blocks(stage_id), clip_scale.reshape(1), sorted_ids, low, g_wide, g_own, g_far, embed_table, mom_embed, vel_embed, low_scale)

        next_in, next_out = new_first.astype(jnp.bfloat16), new_second.astype(jnp.bfloat16)
        next_in0, next_in1 = by_stage(next_in, other(next_in))
        next_out0, next_out1 = by_stage(next_out, other(next_out))
        n_micro, tokens = next_tokens.shape
        my_micro = n_micro // n_stage
        my_rows = lax.dynamic_slice_in_dim(next_tokens, stage_id * my_micro, my_micro).reshape(2, -1)
        gathered = []
        for piece in range(2):
            final_act = next_forward(my_rows[piece], new_embed, next_in0, next_out0, next_in1, next_out1, scale_in)
            gathered.append(lax.all_gather(final_act.reshape(my_micro // 2, tokens, d_model), 'stage', axis=0, tiled=False))
        next_acts = jnp.stack(gathered, axis=1).reshape(n_micro, tokens, d_model)
        return (new_first[None], new_second[None], new_mom_first[None], new_mom_second[None],
                new_vel_first[None], new_vel_second[None], new_embed, new_mom_embed, new_vel_embed, next_acts)

    return jax.shard_map(local_step, mesh=mesh, in_specs=in_specs, out_specs=out_specs, check_vma=False)
```

```python
import functools
import math
import jax
import jax.numpy as jnp
from jax import lax
from jax.experimental import pallas as pl
from jax.experimental.pallas import tpu as pltpu
from jax.sharding import PartitionSpec as P

STEP_COUNT = 10
LEARN_RATE = 1e-3
ADAM_BETA1 = 0.9
ADAM_BETA2 = 0.95
ADAM_EPS = 1e-8
WEIGHT_DECAY = 0.1
CLIP_EPS = 1e-6

TILE = 512
ADAM_TILE = 1024
CHUNK = 512
SEG = 256
TOKEN_BLOCK = 512
FF_CHUNK = 512
FWD_CHUNK = 1024
N_DEV = 8
MESH_ID = pl.DeviceIdType.MESH
WIDE_TILES = 5
NEG = -1e30
GELU_K = math.sqrt(2.0 / math.pi)
GELU_A = 0.044715
BOTH = ('data', 'stage')


def block_forward(act_in, w_in, w_out):
    pre_act = jnp.dot(act_in, w_in, preferred_element_type=jnp.float32)
    hidden = jax.nn.gelu(pre_act).astype(jnp.bfloat16)
    mlp_out = jnp.dot(hidden, w_out, preferred_element_type=jnp.float32)
    return (act_in.astype(jnp.float32) + mlp_out).astype(jnp.bfloat16)


def backward_kernel(n_chunks, g_ref, x_ref, wi_ref, wo_ref, dx_ref, dwi_ref, dwo_ref, back_ref, acc_i, acc_o):
    f = pl.program_id(0)
    wi = wi_ref[...]
    wi_flip = wi.T
    acc_i[...] = jnp.zeros_like(acc_i)
    acc_o[...] = jnp.zeros_like(acc_o)

    @pl.when(f == 0)
    def _():
        back_ref[...] = jnp.zeros_like(back_ref)

    def chunk(c, _):
        rows = pl.ds(pl.multiple_of(c * CHUNK, CHUNK), CHUNK)
        x, g = x_ref[rows, :], g_ref[rows, :]
        pre = dot_last(wi_flip, x)
        d_hidden = dot_last(wo_ref[...], g)
        square = pre * pre
        bend = jnp.tanh(GELU_K * pre * (1.0 + GELU_A * square))
        rise = 0.5 * (1.0 + bend)
        hidden = (pre * rise).astype(jnp.bfloat16)
        slope = rise + (0.5 * GELU_K) * pre * (1.0 - bend * bend) * (1.0 + (3.0 * GELU_A) * square)
        d_pre = (d_hidden * slope).astype(jnp.bfloat16)
        acc_o[...] += jnp.dot(hidden, g, preferred_element_type=jnp.float32)
        acc_i[...] += jnp.dot(d_pre, x, preferred_element_type=jnp.float32)
        back_ref[c] += jnp.dot(wi, d_pre, preferred_element_type=jnp.float32)
        return 0

    lax.fori_loop(0, n_chunks, chunk, 0, unroll=2)
    dwo_ref[...] = acc_o[...]
    dwi_ref[...] = acc_i[...].T

    @pl.when(f == pl.num_programs(0) - 1)
    def _():
        def last(c, _):
            rows = pl.ds(pl.multiple_of(c * CHUNK, CHUNK), CHUNK)
            dx_ref[rows, :] = (g_ref[rows, :].astype(jnp.float32) + back_ref[c].T).astype(jnp.bfloat16)
            return 0
        lax.fori_loop(0, n_chunks, last, 0)


def block_backward(d_out, act_in, w_in, w_out):
    n_tok, d_model = act_in.shape
    ff = w_in.shape[1]
    n_chunks = n_tok // CHUNK
    tokens = pl.BlockSpec((n_tok, d_model), lambda f: (0, 0))
    cols = pl.BlockSpec((d_model, FF_CHUNK), lambda f: (0, f))
    rows = pl.BlockSpec((FF_CHUNK, d_model), lambda f: (f, 0))
    return pl.pallas_call(
        functools.partial(backward_kernel, n_chunks),
        out_shape=[jax.ShapeDtypeStruct((n_tok, d_model), jnp.bfloat16), jax.ShapeDtypeStruct((d_model, ff), jnp.float32),
                   jax.ShapeDtypeStruct((ff, d_model), jnp.float32)],
        grid=(ff // FF_CHUNK,),
        in_specs=[tokens, tokens, cols, rows],
        out_specs=[tokens, cols, rows],
        scratch_shapes=[pltpu.VMEM((n_chunks, d_model, CHUNK), jnp.float32), pltpu.VMEM((FF_CHUNK, d_model), jnp.float32),
                        pltpu.VMEM((FF_CHUNK, d_model), jnp.float32)],
        compiler_params=params(),
        cost_estimate=pl.CostEstimate(flops=10 * n_tok * d_model * ff, bytes_accessed=12 * d_model * ff, transcendentals=0),
        name='block_backward',
    )(d_out, act_in, w_in, w_out)


def adamw_update(master, moment, velocity, gradient, clip_scale):
    scaled_grad = clip_scale * gradient
    moment_new = ADAM_BETA1 * moment + (1.0 - ADAM_BETA1) * scaled_grad
    velocity_new = ADAM_BETA2 * velocity + (1.0 - ADAM_BETA2) * scaled_grad * scaled_grad
    moment_hat = moment_new / (1.0 - ADAM_BETA1 ** STEP_COUNT)
    velocity_hat = velocity_new / (1.0 - ADAM_BETA2 ** STEP_COUNT)
    master_new = master - LEARN_RATE * (moment_hat / (jnp.sqrt(velocity_hat) + ADAM_EPS) + WEIGHT_DECAY * master)
    return master_new, moment_new, velocity_new


def dot_last(a, b):
    return lax.dot_general(a, b, (((1,), (1,)), ((), ())), preferred_element_type=jnp.float32)


def params(limit_mib=60, **kw):
    return pltpu.CompilerParams(vmem_limit_bytes=limit_mib * 1024 * 1024, **kw)


def load_rows(block, e_ref, vocab):
    rows = block * TILE + lax.broadcasted_iota(jnp.int32, (TILE, 1), 0)
    valid = rows < vocab
    e_tile = jnp.where(valid, e_ref[...], 0.0).astype(jnp.bfloat16)
    return rows, valid, e_tile, jnp.where(valid, 0.0, NEG)


def tile_of(n_own, blk_ref, j):
    return jnp.where(j < n_own, blk_ref[0] + j, blk_ref[1] + j)


def stats_kernel(vocab, n_chunks, n_own, blk_ref, z_ref, e_ref, stat_ref):
    _, _, e_tile, bias = load_rows(tile_of(n_own, blk_ref, pl.program_id(0)), e_ref, vocab)

    @pl.when(pl.program_id(0) == 0)
    def _():
        stat_ref[0:1, :] = jnp.full((1, stat_ref.shape[1]), NEG, jnp.float32)
        stat_ref[1:2, :] = jnp.zeros((1, stat_ref.shape[1]), jnp.float32)

    def chunk(c, _):
        cols = pl.ds(pl.multiple_of(c * CHUNK, CHUNK), CHUNK)
        logits = dot_last(e_tile, z_ref[cols, :]) + bias
        top_old = stat_ref[0:1, cols]
        top_new = jnp.maximum(top_old, jnp.max(logits, axis=0, keepdims=True))
        part = jnp.sum(jnp.exp(logits - top_new), axis=0, keepdims=True)
        stat_ref[0:1, cols] = top_new
        stat_ref[1:2, cols] = stat_ref[1:2, cols] * jnp.exp(top_old - top_new) + part
        return 0

    lax.fori_loop(0, n_chunks, chunk, 0, unroll=4)


def head_stats(z_all, embed_table, blocks, n_own, n_tiles):
    vocab, d_model = embed_table.shape
    n_tok = z_all.shape[0]
    last = (vocab - 1) // TILE
    return pl.pallas_call(
        functools.partial(stats_kernel, vocab, n_tok // CHUNK, n_own),
        out_shape=jax.ShapeDtypeStruct((2, n_tok), jnp.float32),
        grid_spec=pltpu.PrefetchScalarGridSpec(
            num_scalar_prefetch=1, grid=(n_tiles,),
            in_specs=[pl.BlockSpec((n_tok, d_model), lambda j, b: (0, 0)),
                      pl.BlockSpec((TILE, d_model), lambda j, b: (jnp.minimum(tile_of(n_own, b, j), last), 0))],
            out_specs=pl.BlockSpec((2, n_tok), lambda j, b: (0, 0))),
        compiler_params=params(),
        cost_estimate=pl.CostEstimate(flops=2 * n_tiles * TILE * n_tok * d_model, bytes_accessed=n_tiles * TILE * d_model * 4, transcendentals=0),
        name='head_stats',
    )(blocks, z_all, embed_table)


def head_kernel(vocab, n_chunks, n_rep, n_own, with_top, blk_ref, z_ref, norm_ref, tgt_ref, e_ref, g_ref, out_ref, *rest):
    top_ref = rest[1] if with_top else None
    acc_ref = rest[-1]
    j = pl.program_id(0)
    rows, valid, e_tile, bias = load_rows(tile_of(n_own, blk_ref, j), e_ref, vocab)
    if with_top:
        e_flip = e_tile.T

        @pl.when(j == 0)
        def _():
            top_ref[...] = jnp.zeros_like(top_ref)

    def chunk(with_rows, c, _):
        cols = pl.ds(pl.multiple_of(c * CHUNK, CHUNK), CHUNK)
        z_chunk = z_ref[cols, :]
        logits = dot_last(e_tile, z_chunk) + bias
        probs = jnp.exp(logits - norm_ref[0:1, cols]) * norm_ref[1:2, cols]
        d_logits = jnp.where(rows == tgt_ref[0:1, cols], probs - 1.0, probs).astype(jnp.bfloat16)
        if with_rows:
            acc_ref[...] += jnp.dot(d_logits, z_chunk, preferred_element_type=jnp.float32)
        if with_top:
            top_ref[c] += jnp.dot(e_flip, d_logits, preferred_element_type=jnp.float32)
        return 0

    @pl.when(j < n_own)
    def _():
        acc_ref[...] = jnp.zeros_like(acc_ref)
        lax.fori_loop(0, n_chunks, functools.partial(chunk, True), 0, unroll=2 if with_top else 4)
        out_ref[...] = jnp.where(valid, g_ref[...], 0.0) + acc_ref[...] * (1.0 / n_rep)

    if with_top:
        @pl.when(j >= n_own)
        def _():
            lax.fori_loop(0, n_chunks, functools.partial(chunk, False), 0, unroll=2)

        @pl.when(j == pl.num_programs(0) - 1)
        def _():
            def turn(c, _):
                rest[0][c] = top_ref[c].T
                return 0
            lax.fori_loop(0, n_chunks, turn, 0)


def head_grads(z_all, norm, targets, embed_table, grad_embed, blocks, n_own, n_tiles, n_rep, with_top):
    vocab, d_model = embed_table.shape
    n_tok = z_all.shape[0]
    n_chunks = n_tok // CHUNK
    last = (vocab - 1) // TILE
    out_shape = [jax.ShapeDtypeStruct((n_own * TILE, d_model), jnp.float32)]
    out_specs = [pl.BlockSpec((TILE, d_model), lambda j, b: (jnp.minimum(j, n_own - 1), 0))]
    if with_top:
        out_shape.append(jax.ShapeDtypeStruct((n_chunks, CHUNK, d_model), jnp.float32))
        out_specs.append(pl.BlockSpec((n_chunks, CHUNK, d_model), lambda j, b: (0, 0, 0), pipeline_mode=pl.Buffered(1)))
    return pl.pallas_call(
        functools.partial(head_kernel, vocab, n_chunks, n_rep, n_own, with_top),
        out_shape=out_shape,
        grid_spec=pltpu.PrefetchScalarGridSpec(
            num_scalar_prefetch=1, grid=(n_tiles,),
            in_specs=[pl.BlockSpec((n_tok, d_model), lambda j, b: (0, 0)),
                      pl.BlockSpec((2, n_tok), lambda j, b: (0, 0)),
                      pl.BlockSpec((1, n_tok), lambda j, b: (0, 0)),
                      pl.BlockSpec((TILE, d_model), lambda j, b: (jnp.minimum(tile_of(n_own, b, j), last), 0)),
                      pl.BlockSpec((TILE, d_model), lambda j, b: (jnp.minimum(b[0] + jnp.minimum(j, n_own - 1), last), 0))],
            out_specs=out_specs,
            scratch_shapes=[pltpu.VMEM((n_chunks, d_model, CHUNK), jnp.float32)] * with_top + [pltpu.VMEM((TILE, d_model), jnp.float32)]),
        compiler_params=params(),
        cost_estimate=pl.CostEstimate(flops=(6 if with_top else 4) * n_tiles * TILE * n_tok * d_model,
                                      bytes_accessed=n_tiles * TILE * d_model * 12, transcendentals=0),
        name='head_grads' if with_top else 'head_rows',
    )(blocks, z_all, norm, targets, embed_table, grad_embed)


def sparse_rows(block, start_ref, ids_ref, low_ref, base):
    rows = block * TILE + lax.broadcasted_iota(jnp.int32, (TILE, 1), 0)
    first = start_ref[block] // SEG
    stop = (start_ref[block + 1] + SEG - 1) // SEG

    def segment(c, acc):
        pick = jnp.where(rows == ids_ref[pl.ds(c, 1), :], 1.0, 0.0).astype(jnp.bfloat16)
        return acc + jnp.dot(pick, low_ref[pl.ds(pl.multiple_of(c * SEG, SEG), SEG), :], preferred_element_type=jnp.float32)

    return lax.fori_loop(first, stop, segment, base)


def sumsq_kernel(low_scale, blk_ref, start_ref, ids_ref, low_ref, g_ref, out_ref):
    block = blk_ref[0] + pl.program_id(0)
    zero = jnp.zeros(g_ref.shape, jnp.float32)
    full = g_ref[...] + low_scale * sparse_rows(block, start_ref, ids_ref, low_ref, zero)

    @pl.when(pl.program_id(0) == 0)
    def _():
        out_ref[...] = jnp.zeros_like(out_ref)

    out_ref[...] += jnp.sum((full * full).reshape(-1, 8, full.shape[1]), axis=0)


def rows_sumsq(blocks, starts, ids, low, g_rows, n_tiles, low_scale):
    d_model = g_rows.shape[1]
    return pl.pallas_call(
        functools.partial(sumsq_kernel, low_scale),
        out_shape=jax.ShapeDtypeStruct((8, d_model), jnp.float32),
        grid_spec=pltpu.PrefetchScalarGridSpec(
            num_scalar_prefetch=2, grid=(n_tiles,),
            in_specs=[pl.BlockSpec(ids.shape, lambda j, b, s: (0, 0)),
                      pl.BlockSpec(low.shape, lambda j, b, s: (0, 0)),
                      pl.BlockSpec((TILE, d_model), lambda j, b, s: (b[1] + j, 0))],
            out_specs=pl.BlockSpec((8, d_model), lambda j, b, s: (0, 0))),
        compiler_params=params(),
        name='rows_sumsq',
    )(blocks, starts, ids, low, g_rows)


def adam_kernel(low_scale, n_wide, n_red, start_ref, stage_ref, clip_ref, ids_ref, low_ref, gw_ref, go_ref, gf_ref,
                w_ref, m_ref, v_ref, w_out, m_out, v_out, acc_ref):
    j = pl.program_id(0)
    own = n_wide + n_red * stage_ref[0]
    is_own = (j >= own) & (j < own + n_red)

    rows = j * ADAM_TILE + lax.broadcasted_iota(jnp.int32, (ADAM_TILE, 1), 0)
    per = ADAM_TILE // TILE
    first = jnp.minimum(start_ref[per * j] // SEG, ids_ref.shape[0] - 1)

    def segment(c):
        pick = jnp.where(rows == ids_ref[pl.ds(c, 1), :], 1.0, 0.0).astype(jnp.bfloat16)
        return low_scale * jnp.dot(pick, low_ref[pl.ds(pl.multiple_of(c * SEG, SEG), SEG), :], preferred_element_type=jnp.float32)

    @pl.when(j < n_wide)
    def _():
        acc_ref[...] = gw_ref[...] + segment(first)

    @pl.when(is_own)
    def _():
        acc_ref[...] = go_ref[...] + segment(first)

    @pl.when((j >= n_wide) & jnp.logical_not(is_own))
    def _():
        acc_ref[...] = gf_ref[...] + segment(first)

    def add(c, _):
        acc_ref[...] += segment(c)
        return 0

    lax.fori_loop(first + 1, (start_ref[per * j + per] + SEG - 1) // SEG, add, 0)

    def part(i, _):
        r = pl.ds(pl.multiple_of(i * 32, 32), 32)
        w_new, m_new, v_new = adamw_update(w_ref[r, :], m_ref[r, :], v_ref[r, :], acc_ref[r, :], clip_ref[0])
        w_out[r, :] = w_new
        m_out[r, :] = m_new
        v_out[r, :] = v_new
        return 0

    lax.fori_loop(0, ADAM_TILE // 32, part, 0)


def embed_adam(starts, stage, clip, ids, low, g_wide, g_own, g_far, embed_table, mom, vel, low_scale):
    vocab, d_model = embed_table.shape
    n_wide, n_red = g_wide.shape[0] // ADAM_TILE, g_own.shape[0] // ADAM_TILE
    spec = pl.BlockSpec((ADAM_TILE, d_model), lambda j, s, t, c: (j, 0))
    shape = jax.ShapeDtypeStruct((vocab, d_model), jnp.float32)

    def held(first):
        return pl.BlockSpec((ADAM_TILE, d_model), lambda j, s, t, c: (jnp.clip(j - n_wide - n_red * first(t[0]), 0, n_red - 1), 0))

    return pl.pallas_call(
        functools.partial(adam_kernel, low_scale, n_wide, n_red),
        out_shape=[shape] * 3,
        grid_spec=pltpu.PrefetchScalarGridSpec(
            num_scalar_prefetch=3, grid=(pl.cdiv(vocab, ADAM_TILE),),
            in_specs=[pl.BlockSpec(ids.shape, lambda j, s, t, c: (0, 0)),
                      pl.BlockSpec(low.shape, lambda j, s, t, c: (0, 0)),
                      pl.BlockSpec((ADAM_TILE, d_model), lambda j, s, t, c: (jnp.minimum(j, n_wide - 1), 0)),
                      held(lambda t: t), held(lambda t: 1 - t), spec, spec, spec],
            out_specs=[spec] * 3,
            scratch_shapes=[pltpu.VMEM((ADAM_TILE, d_model), jnp.float32)]),
        compiler_params=params(),
        cost_estimate=pl.CostEstimate(flops=20 * vocab * d_model, bytes_accessed=28 * vocab * d_model, transcendentals=0),
        name='embed_adam',
    )(starts, stage, clip, ids, low, g_wide, g_own, g_far, embed_table, mom, vel)


def next_kernel(scale, n_blocks, ids_ref, table_ref, wi0_ref, wo0_ref, wi1_ref, wo1_ref, out_ref, rows_ref, x_ref, acc_ref, sems):
    blk = pl.program_id(0)
    slot = lax.rem(blk, 2)
    n_ff = wi0_ref.shape[1] // FWD_CHUNK
    per = TOKEN_BLOCK // (2 * n_ff)

    def fetch(base, to_slot, first, count):
        for t in range(count):
            row = ids_ref[base + first + t]
            pltpu.make_async_copy(table_ref.at[pl.ds(row, 1), :], rows_ref.at[to_slot, pl.ds(first + t, 1), :], sems.at[to_slot]).start()

    @pl.when(blk == 0)
    def _():
        def step(i, _):
            fetch(0, 0, i * 16, 16)
            return 0
        lax.fori_loop(0, TOKEN_BLOCK // 16, step, 0)

    pltpu.make_async_copy(rows_ref.at[1 - slot], rows_ref.at[slot], sems.at[slot]).wait()
    base = jnp.minimum(blk + 1, n_blocks - 1) * TOKEN_BLOCK
    x_ref[...] = (scale * rows_ref[slot].astype(jnp.bfloat16).astype(jnp.float32)).astype(jnp.bfloat16)

    for layer, (wi_ref, wo_ref) in enumerate(((wi0_ref, wo0_ref), (wi1_ref, wo1_ref))):
        acc_ref[...] = x_ref[...].astype(jnp.float32)
        for c in range(n_ff):
            fetch(base, 1 - slot, (layer * n_ff + c) * per, per)
            cols = pl.ds(c * FWD_CHUNK, FWD_CHUNK)
            pre_act = jnp.dot(x_ref[...], wi_ref[:, cols], preferred_element_type=jnp.float32)
            bend = jnp.tanh(pre_act * (GELU_K + (GELU_K * GELU_A) * (pre_act * pre_act)))
            hidden = ((0.5 * pre_act) * (1.0 + bend)).astype(jnp.bfloat16)
            acc_ref[...] += jnp.dot(hidden, wo_ref[cols, :], preferred_element_type=jnp.float32)
        if layer == 0:
            x_ref[...] = acc_ref[...].astype(jnp.bfloat16)
        else:
            out_ref[...] = acc_ref[...].astype(jnp.bfloat16)

    @pl.when(blk == n_blocks - 1)
    def _():
        pltpu.make_async_copy(rows_ref.at[slot], rows_ref.at[1 - slot], sems.at[1 - slot]).wait()


def next_forward(ids, table, wi0, wo0, wi1, wo1, scale):
    n_tok = ids.shape[0]
    d_model = table.shape[1]
    whole = [pl.BlockSpec(w.shape, lambda j, s: (0, 0)) for w in (wi0, wo0, wi1, wo1)]
    return pl.pallas_call(
        functools.partial(next_kernel, scale, n_tok // TOKEN_BLOCK),
        out_shape=jax.ShapeDtypeStruct((n_tok, d_model), jnp.bfloat16),
        grid_spec=pltpu.PrefetchScalarGridSpec(
            num_scalar_prefetch=1, grid=(n_tok // TOKEN_BLOCK,),
            in_specs=[pl.BlockSpec(memory_space=pl.ANY)] + whole,
            out_specs=pl.BlockSpec((TOKEN_BLOCK, d_model), lambda j, s: (j, 0)),
            scratch_shapes=[pltpu.VMEM((2, TOKEN_BLOCK, d_model), jnp.float32), pltpu.VMEM((TOKEN_BLOCK, d_model), jnp.bfloat16),
                            pltpu.VMEM((TOKEN_BLOCK, d_model), jnp.float32), pltpu.SemaphoreType.DMA((2,))]),
        compiler_params=params(),
        cost_estimate=pl.CostEstimate(flops=8 * n_tok * d_model * wi0.shape[1], bytes_accessed=6 * n_tok * d_model, transcendentals=0),
        name='next_forward',
    )(ids, table, wi0, wo0, wi1, wo1)


def exchange(x_ref, all_ref, send_sems, recv_sems):
    n_stage = lax.axis_size('stage')
    me = lax.axis_index('data') * n_stage + lax.axis_index('stage')

    def place(k):
        to = lax.rem(me + k, N_DEV)
        return to // n_stage, lax.rem(to, n_stage)

    barrier = pltpu.get_barrier_semaphore()
    for k in range(1, N_DEV):
        pl.semaphore_signal(barrier, inc=1, device_id=place(k), device_id_type=MESH_ID)
    pl.semaphore_wait(barrier, N_DEV - 1)
    copies = []
    for k in range(1, N_DEV):
        copies.append(pltpu.make_async_remote_copy(
            src_ref=x_ref, dst_ref=all_ref.at[k - 1], send_sem=send_sems.at[k - 1], recv_sem=recv_sems.at[k - 1],
            device_id=place(k), device_id_type=MESH_ID))
        copies[-1].start()
    for copy in copies:
        copy.wait()


def norm_kernel(x_ref, out_ref, all_ref, send_sems, recv_sems):
    exchange(x_ref, all_ref, send_sems, recv_sems)
    top = x_ref[0:1, :]
    for k in range(N_DEV - 1):
        top = jnp.maximum(top, all_ref[k, 0:1, :])
    total = x_ref[1:2, :] * jnp.exp(x_ref[0:1, :] - top)
    for k in range(N_DEV - 1):
        total += all_ref[k, 1:2, :] * jnp.exp(all_ref[k, 0:1, :] - top)
    out_ref[0:1, :] = top
    out_ref[1:2, :] = 1.0 / total


def gather_kernel(x_ref, out_ref, all_ref, send_sems, recv_sems):
    exchange(x_ref, all_ref, send_sems, recv_sems)
    me = lax.axis_index('data') * lax.axis_size('stage') + lax.axis_index('stage')
    out_ref[pl.ds(me, 1)] = x_ref[...][None]
    for k in range(N_DEV - 1):
        out_ref[pl.ds(lax.rem(me + (N_DEV - 1 - k), N_DEV), 1)] = all_ref[k:k + 1]


def small_exchange(body, x, out_shape, collective_id, name):
    return pl.pallas_call(
        body,
        out_shape=out_shape,
        in_specs=[pl.BlockSpec(memory_space=pltpu.VMEM)],
        out_specs=pl.BlockSpec(memory_space=pltpu.VMEM),
        scratch_shapes=[pltpu.VMEM((N_DEV - 1,) + x.shape, x.dtype), pltpu.SemaphoreType.DMA((N_DEV - 1,)),
                        pltpu.SemaphoreType.DMA((N_DEV - 1,))],
        compiler_params=pltpu.CompilerParams(collective_id=collective_id, has_side_effects=True),
        name=name,
    )(x)


def solution(mesh):
    n_stage = mesh.shape['stage']
    n_rep = mesh.shape['data']
    n_dev = n_stage * n_rep
    swap = [(0, 1), (1, 0)]
    w_spec = P('stage', None, None)
    in_specs = (w_spec,) * 8 + (P(None, None),) * 4 + (P('stage', 'data', None), P('data'), P('data'), P(None, 'data'), P(None))
    out_specs = (w_spec,) * 6 + (P(None, None),) * 3 + (P(None, 'data', None),)

    def local_step(w_first, w_second, mom_first, mom_second, vel_first, vel_second, grad_first, grad_second,
                   embed_table, mom_embed, vel_embed, grad_embed, stage_acts, last_tokens, targets, next_tokens, max_norm):
        stage_id = lax.axis_index('stage')
        dev_id = lax.axis_index('data') * n_stage + stage_id
        low_core = stage_id == 0
        vocab, d_model = embed_table.shape
        scale_in = math.sqrt(d_model)
        low_scale = scale_in / n_rep
        n_tiles = -(-vocab // (TILE * n_dev))
        n_wide = WIDE_TILES
        n_rest = n_tiles - n_wide
        n_red = n_rest * n_dev // n_stage
        n_part = n_red // n_rep
        rest0 = n_dev * n_wide

        def other(x):
            return lax.ppermute(x, 'stage', swap)

        def by_stage(own, far):
            return jnp.where(low_core, own, far), jnp.where(low_core, far, own)

        w_in, w_out = w_first[0].astype(jnp.bfloat16), w_second[0].astype(jnp.bfloat16)
        w_in0, w_in1 = by_stage(w_in, other(w_in))
        w_out0, w_out1 = by_stage(w_out, other(w_out))

        z_own = block_forward(stage_acts[0], w_in, w_out)
        cut = z_own.shape[0] // 2
        z_piece = jnp.where(low_core, lax.ppermute(z_own[:cut], 'stage', [(1, 0)]), z_own[cut:])
        all_ids = lax.all_gather(jnp.stack([last_tokens, targets]), 'data', axis=1, tiled=True)
        ids, tgts = all_ids[0], all_ids[1:2]
        n_tok = ids.shape[0]
        half = n_tok // 2
        z_all = lax.all_gather(z_piece, BOTH, axis=0, tiled=True)

        order = jnp.arange(n_tok, dtype=jnp.int32)
        before = (ids[None, :] < ids[:, None]) | ((ids[None, :] == ids[:, None]) & (order[None, :] < order[:, None]))
        rank = jnp.sum(before.astype(jnp.int32), axis=1)
        edges = TILE * jnp.arange(n_tiles * n_dev + 1, dtype=jnp.int32)
        starts = jnp.sum((ids[None, :] < edges[:, None]).astype(jnp.int32), axis=1)
        z_all, rank, starts, acts_in = lax.optimization_barrier((z_all, rank, starts, stage_acts[0]))

        acts = lax.all_gather(acts_in, 'data', axis=0, tiled=True)

        def blocks(*tiles):
            return jnp.stack([jnp.asarray(t, jnp.int32) for t in tiles])

        shard = blocks(dev_id * n_wide, rest0 + dev_id * n_rest - n_wide)
        stat = head_stats(z_all, embed_table, shard, n_wide, n_tiles)
        norm = small_exchange(norm_kernel, stat, jax.ShapeDtypeStruct(stat.shape, jnp.float32), 1, 'share_stats')
        norm, acts = lax.optimization_barrier((norm, acts))
        mine = lax.dynamic_slice_in_dim(acts, stage_id * half, half)
        far = other(lax.dynamic_slice_in_dim(acts, (1 - stage_id) * half, half))
        act0, act1 = by_stage(mine, far)
        g_shard, d_top_part = head_grads(z_all, norm, tgts, embed_table, grad_embed, shard, n_wide, n_tiles, n_rep, True)
        d_top_own = lax.psum_scatter(d_top_part, BOTH, scatter_dimension=0, tiled=True)
        red_tile = rest0 + stage_id * n_red
        g_own = head_grads(z_all, norm, tgts, embed_table, grad_embed, blocks(red_tile, red_tile), n_red, n_red, n_rep, False)[0]
        d_top_own, g_own = lax.optimization_barrier((d_top_own, g_own))
        d_top_own = d_top_own.reshape(-1, d_model).astype(jnp.bfloat16)
        g_shard, d_top_own, late_ids = lax.optimization_barrier((g_shard, d_top_own, ids))
        d_top = lax.all_gather(d_top_own, BOTH, axis=0, tiled=True)
        sorted_ids = jnp.sum(jnp.where(rank[None, :] == order[:, None], late_ids[None, :], 0), axis=1).reshape(n_tok // SEG, SEG)
        d_top, sorted_ids = lax.optimization_barrier((d_top, sorted_ids))
        g_far = other(g_own)
        g_wide = lax.all_gather(g_shard, BOTH, axis=0, tiled=True)

        d_half = lax.dynamic_slice_in_dim(d_top, stage_id * half, half)
        d_act1, g_in1, g_out1 = block_backward(d_half, act1, w_in1, w_out1)
        d_low_half, g_in0, g_out0 = block_backward(d_act1, act0, w_in0, w_out0)
        my_rank = lax.dynamic_slice_in_dim(rank, stage_id * half, half)
        perm = (my_rank[None, :] == order[:, None]).astype(jnp.bfloat16)
        low_half = jnp.dot(perm, d_low_half, preferred_element_type=jnp.float32).astype(jnp.bfloat16)
        low = low_half + other(low_half)

        def both_halves(part0, part1):
            far0, far1 = lax.ppermute(part0, 'stage', [(1, 0)]), lax.ppermute(part1, 'stage', [(0, 1)])
            return jnp.where(low_core, part0 + far0, part1 + far1)

        full_first = grad_first[0] + both_halves(g_in0, g_in1) / n_rep
        full_second = grad_second[0] + both_halves(g_out0, g_out1) / n_rep
        my_part = lax.axis_index('data') * n_part
        embed_sq = (jnp.sum(rows_sumsq(blocks(dev_id * n_wide, 0), starts, sorted_ids, low, g_shard, n_wide, low_scale))
                    + jnp.sum(rows_sumsq(blocks(red_tile + my_part, my_part), starts, sorted_ids, low, g_own, n_part, low_scale)))
        stage_sq = jnp.sum(full_first * full_first) + jnp.sum(full_second * full_second)
        own_sq = jnp.full((8, 128), embed_sq + stage_sq / n_rep)
        all_sq = small_exchange(gather_kernel, own_sq, jax.ShapeDtypeStruct((n_dev, 8, 128), jnp.float32), 2, 'share_sums')
        total_sq = jnp.sum(all_sq[:, 0, 0])
        clip_scale = jnp.minimum(1.0, max_norm[0] / (jnp.sqrt(total_sq) + CLIP_EPS))
        new_first, new_mom_first, new_vel_first = adamw_update(w_first[0], mom_first[0], vel_first[0], full_first, clip_scale)
        new_second, new_mom_second, new_vel_second = adamw_update(w_second[0], mom_second[0], vel_second[0], full_second, clip_scale)
        new_embed, new_mom_embed, new_vel_embed = embed_adam(
            starts, blocks(stage_id), clip_scale.reshape(1), sorted_ids, low, g_wide, g_own, g_far, embed_table, mom_embed, vel_embed, low_scale)

        next_in, next_out = new_first.astype(jnp.bfloat16), new_second.astype(jnp.bfloat16)
        next_in0, next_in1 = by_stage(next_in, other(next_in))
        next_out0, next_out1 = by_stage(next_out, other(next_out))
        n_micro, tokens = next_tokens.shape
        my_micro = n_micro // n_stage
        my_rows = lax.dynamic_slice_in_dim(next_tokens, stage_id * my_micro, my_micro).reshape(2, -1)
        gathered = []
        for piece in range(2):
            final_act = next_forward(my_rows[piece], new_embed, next_in0, next_out0, next_in1, next_out1, scale_in)
            gathered.append(lax.all_gather(final_act.reshape(my_micro // 2, tokens, d_model), 'stage', axis=0, tiled=False))
        next_acts = jnp.stack(gathered, axis=1).reshape(n_micro, tokens, d_model)
        return (new_first[None], new_second[None], new_mom_first[None], new_mom_second[None],
                new_vel_first[None], new_vel_second[None], new_embed, new_mom_embed, new_vel_embed, next_acts)

    return jax.shard_map(local_step, mesh=mesh, in_specs=in_specs, out_specs=out_specs, check_vma=False)
```

```python
import functools
import math
import jax
import jax.numpy as jnp
from jax import lax
from jax.experimental import pallas as pl
from jax.experimental.pallas import tpu as pltpu
from jax.sharding import PartitionSpec as P

STEP_COUNT = 10
LEARN_RATE = 1e-3
ADAM_BETA1 = 0.9
ADAM_BETA2 = 0.95
ADAM_EPS = 1e-8
WEIGHT_DECAY = 0.1
CLIP_EPS = 1e-6

TILE = 512
ADAM_TILE = 1024
CHUNK = 512
SEG = 256
TOKEN_BLOCK = 512
FF_CHUNK = 512
FWD_CHUNK = 1024
N_DEV = 8
MESH_ID = pl.DeviceIdType.MESH
WIDE_TILES = 5
NEG = -1e30
GELU_K = math.sqrt(2.0 / math.pi)
GELU_A = 0.044715
BOTH = ('data', 'stage')


def block_forward(act_in, w_in, w_out):
    pre_act = jnp.dot(act_in, w_in, preferred_element_type=jnp.float32)
    hidden = jax.nn.gelu(pre_act).astype(jnp.bfloat16)
    mlp_out = jnp.dot(hidden, w_out, preferred_element_type=jnp.float32)
    return (act_in.astype(jnp.float32) + mlp_out).astype(jnp.bfloat16)


def backward_kernel(n_chunks, n_ff, n_rep, g_ref, x_ref, wi_ref, wo_ref, old_i_ref, old_o_ref, dx_ref, full_i_ref, full_o_ref, sq_ref,
                    back_ref, part_ref, far_ref, send_sems, recv_sems):
    f = pl.program_id(0)
    partner = (lax.axis_index('data'), 1 - lax.axis_index('stage'))

    def copy(i, which):
        return pltpu.make_async_remote_copy(
            src_ref=part_ref.at[i, which], dst_ref=far_ref.at[i, which], send_sem=send_sems.at[i, which],
            recv_sem=recv_sems.at[i, which], device_id=partner, device_id_type=MESH_ID)

    @pl.when(f == 0)
    def _():
        barrier = pltpu.get_barrier_semaphore()
        pl.semaphore_signal(barrier, inc=1, device_id=partner, device_id_type=MESH_ID)
        pl.semaphore_wait(barrier, 1)
        back_ref[...] = jnp.zeros_like(back_ref)

    for i in range(n_ff - 1):
        @pl.when(f == i + 1)
        def _():
            copy(i, 0).start()
            copy(i, 1).start()

    wi = wi_ref[...]
    wi_flip = wi.T
    part_ref[f] = jnp.zeros(part_ref.shape[1:], jnp.float32)

    def chunk(c, _):
        rows = pl.ds(pl.multiple_of(c * CHUNK, CHUNK), CHUNK)
        x, g = x_ref[rows, :], g_ref[rows, :]
        pre = dot_last(wi_flip, x)
        d_hidden = dot_last(wo_ref[...], g)
        square = pre * pre
        bend = jnp.tanh(GELU_K * pre * (1.0 + GELU_A * square))
        rise = 0.5 * (1.0 + bend)
        hidden = (pre * rise).astype(jnp.bfloat16)
        slope = rise + (0.5 * GELU_K) * pre * (1.0 - bend * bend) * (1.0 + (3.0 * GELU_A) * square)
        d_pre = (d_hidden * slope).astype(jnp.bfloat16)
        part_ref[f, 0] += jnp.dot(d_pre, x, preferred_element_type=jnp.float32)
        part_ref[f, 1] += jnp.dot(hidden, g, preferred_element_type=jnp.float32)
        back_ref[c] += jnp.dot(wi, d_pre, preferred_element_type=jnp.float32)
        return 0

    lax.fori_loop(0, n_chunks, chunk, 0, unroll=2)

    @pl.when(f == n_ff - 1)
    def _():
        sq_ref[...] = jnp.zeros_like(sq_ref)

        def last(c, _):
            rows = pl.ds(pl.multiple_of(c * CHUNK, CHUNK), CHUNK)
            dx_ref[rows, :] = (g_ref[rows, :].astype(jnp.float32) + back_ref[c].T).astype(jnp.bfloat16)
            return 0

        def squares(x):
            sq_ref[...] += jnp.sum((x * x).reshape(-1, 8, x.shape[1]), axis=0)

        lax.fori_loop(0, n_chunks, last, 0)
        copy(n_ff - 1, 0).start()
        copy(n_ff - 1, 1).start()
        for i in range(n_ff):
            part = pl.ds(i * FF_CHUNK, FF_CHUNK)
            copy(i, 0).wait()
            copy(i, 1).wait()
            full_i = old_i_ref[:, part] + (part_ref[i, 0] + far_ref[i, 0]).T * (1.0 / n_rep)
            full_i_ref[:, part] = full_i
            squares(full_i)
            full_o = old_o_ref[part, :] + (part_ref[i, 1] + far_ref[i, 1]) * (1.0 / n_rep)
            full_o_ref[part, :] = full_o
            squares(full_o)


def block_backward(d_out, act_in, w_in, w_out, old_in, old_out, n_rep, collective_id):
    n_tok, d_model = act_in.shape
    ff = w_in.shape[1]
    n_chunks, n_ff = n_tok // CHUNK, ff // FF_CHUNK

    def whole(*shape):
        return pl.BlockSpec(shape, lambda f: (0, 0), pipeline_mode=pl.Buffered(1))

    tokens = whole(n_tok, d_model)
    part = (n_ff, 2, FF_CHUNK, d_model)
    return pl.pallas_call(
        functools.partial(backward_kernel, n_chunks, n_ff, n_rep),
        out_shape=[jax.ShapeDtypeStruct((n_tok, d_model), jnp.bfloat16), jax.ShapeDtypeStruct((d_model, ff), jnp.float32),
                   jax.ShapeDtypeStruct((ff, d_model), jnp.float32), jax.ShapeDtypeStruct((8, d_model), jnp.float32)],
        grid=(n_ff,),
        in_specs=[tokens, tokens, pl.BlockSpec((d_model, FF_CHUNK), lambda f: (0, f)), pl.BlockSpec((FF_CHUNK, d_model), lambda f: (f, 0)),
                  whole(d_model, ff), whole(ff, d_model)],
        out_specs=[tokens, whole(d_model, ff), whole(ff, d_model), whole(8, d_model)],
        scratch_shapes=[pltpu.VMEM((n_chunks, d_model, CHUNK), jnp.float32), pltpu.VMEM(part, jnp.float32), pltpu.VMEM(part, jnp.float32),
                        pltpu.SemaphoreType.DMA((n_ff, 2)), pltpu.SemaphoreType.DMA((n_ff, 2))],
        compiler_params=params(collective_id=collective_id, has_side_effects=True),
        cost_estimate=pl.CostEstimate(flops=10 * n_tok * d_model * ff, bytes_accessed=12 * d_model * ff, transcendentals=0),
        name='block_backward',
    )(d_out, act_in, w_in, w_out, old_in, old_out)


def adamw_update(master, moment, velocity, gradient, clip_scale):
    scaled_grad = clip_scale * gradient
    moment_new = ADAM_BETA1 * moment + (1.0 - ADAM_BETA1) * scaled_grad
    velocity_new = ADAM_BETA2 * velocity + (1.0 - ADAM_BETA2) * scaled_grad * scaled_grad
    moment_hat = moment_new / (1.0 - ADAM_BETA1 ** STEP_COUNT)
    velocity_hat = velocity_new / (1.0 - ADAM_BETA2 ** STEP_COUNT)
    master_new = master - LEARN_RATE * (moment_hat / (jnp.sqrt(velocity_hat) + ADAM_EPS) + WEIGHT_DECAY * master)
    return master_new, moment_new, velocity_new


def dot_last(a, b):
    return lax.dot_general(a, b, (((1,), (1,)), ((), ())), preferred_element_type=jnp.float32)


def params(limit_mib=60, **kw):
    return pltpu.CompilerParams(vmem_limit_bytes=limit_mib * 1024 * 1024, **kw)


def load_rows(block, e_ref, vocab):
    rows = block * TILE + lax.broadcasted_iota(jnp.int32, (TILE, 1), 0)
    valid = rows < vocab
    e_tile = jnp.where(valid, e_ref[...], 0.0).astype(jnp.bfloat16)
    return rows, valid, e_tile, jnp.where(valid, 0.0, NEG)


def tile_of(n_own, blk_ref, j):
    return jnp.where(j < n_own, blk_ref[0] + j, blk_ref[1] + j)


def stats_kernel(vocab, n_chunks, n_own, blk_ref, z_ref, e_ref, stat_ref):
    _, _, e_tile, bias = load_rows(tile_of(n_own, blk_ref, pl.program_id(0)), e_ref, vocab)

    @pl.when(pl.program_id(0) == 0)
    def _():
        stat_ref[0:1, :] = jnp.full((1, stat_ref.shape[1]), NEG, jnp.float32)
        stat_ref[1:2, :] = jnp.zeros((1, stat_ref.shape[1]), jnp.float32)

    def chunk(c, _):
        cols = pl.ds(pl.multiple_of(c * CHUNK, CHUNK), CHUNK)
        logits = dot_last(e_tile, z_ref[cols, :]) + bias
        top_old = stat_ref[0:1, cols]
        top_new = jnp.maximum(top_old, jnp.max(logits, axis=0, keepdims=True))
        part = jnp.sum(jnp.exp(logits - top_new), axis=0, keepdims=True)
        stat_ref[0:1, cols] = top_new
        stat_ref[1:2, cols] = stat_ref[1:2, cols] * jnp.exp(top_old - top_new) + part
        return 0

    lax.fori_loop(0, n_chunks, chunk, 0, unroll=4)


def head_stats(z_all, embed_table, blocks, n_own, n_tiles):
    vocab, d_model = embed_table.shape
    n_tok = z_all.shape[0]
    last = (vocab - 1) // TILE
    return pl.pallas_call(
        functools.partial(stats_kernel, vocab, n_tok // CHUNK, n_own),
        out_shape=jax.ShapeDtypeStruct((2, n_tok), jnp.float32),
        grid_spec=pltpu.PrefetchScalarGridSpec(
            num_scalar_prefetch=1, grid=(n_tiles,),
            in_specs=[pl.BlockSpec((n_tok, d_model), lambda j, b: (0, 0)),
                      pl.BlockSpec((TILE, d_model), lambda j, b: (jnp.minimum(tile_of(n_own, b, j), last), 0))],
            out_specs=pl.BlockSpec((2, n_tok), lambda j, b: (0, 0))),
        compiler_params=params(),
        cost_estimate=pl.CostEstimate(flops=2 * n_tiles * TILE * n_tok * d_model, bytes_accessed=n_tiles * TILE * d_model * 4, transcendentals=0),
        name='head_stats',
    )(blocks, z_all, embed_table)


def head_kernel(vocab, n_chunks, n_rep, n_own, with_top, blk_ref, z_ref, norm_ref, tgt_ref, e_ref, g_ref, out_ref, *rest):
    top_ref = rest[1] if with_top else None
    acc_ref = rest[-1]
    j = pl.program_id(0)
    rows, valid, e_tile, bias = load_rows(tile_of(n_own, blk_ref, j), e_ref, vocab)
    if with_top:
        e_flip = e_tile.T

        @pl.when(j == 0)
        def _():
            top_ref[...] = jnp.zeros_like(top_ref)

    def chunk(with_rows, c, _):
        cols = pl.ds(pl.multiple_of(c * CHUNK, CHUNK), CHUNK)
        z_chunk = z_ref[cols, :]
        logits = dot_last(e_tile, z_chunk) + bias
        probs = jnp.exp(logits - norm_ref[0:1, cols]) * norm_ref[1:2, cols]
        d_logits = jnp.where(rows == tgt_ref[0:1, cols], probs - 1.0, probs).astype(jnp.bfloat16)
        if with_rows:
            acc_ref[...] += jnp.dot(d_logits, z_chunk, preferred_element_type=jnp.float32)
        if with_top:
            top_ref[c] += jnp.dot(e_flip, d_logits, preferred_element_type=jnp.float32)
        return 0

    @pl.when(j < n_own)
    def _():
        acc_ref[...] = jnp.zeros_like(acc_ref)
        lax.fori_loop(0, n_chunks, functools.partial(chunk, True), 0, unroll=2 if with_top else 4)
        out_ref[...] = jnp.where(valid, g_ref[...], 0.0) + acc_ref[...] * (1.0 / n_rep)

    if with_top:
        @pl.when(j >= n_own)
        def _():
            lax.fori_loop(0, n_chunks, functools.partial(chunk, False), 0, unroll=2)

        @pl.when(j == pl.num_programs(0) - 1)
        def _():
            def turn(c, _):
                rest[0][c] = top_ref[c].T
                return 0
            lax.fori_loop(0, n_chunks, turn, 0)


def head_rows(z_all, norm, targets, embed_table, grad_embed, blocks, n_own, first, n_tiles, n_rep, held=None):
    vocab, d_model = embed_table.shape
    n_tok = z_all.shape[0]
    last = (vocab - 1) // TILE
    rows = pl.BlockSpec((TILE, d_model), lambda j, b: (jnp.minimum(b[0] + j, last), 0))

    def kernel(blk_ref, z_ref, norm_ref, tgt_ref, e_ref, g_ref, *rest):
        head_kernel(vocab, n_tok // CHUNK, n_rep, n_own, False, blk_ref, z_ref, norm_ref, tgt_ref, e_ref, g_ref, *rest[-2:])

    return pl.pallas_call(
        kernel,
        out_shape=jax.ShapeDtypeStruct((n_own * TILE, d_model), jnp.float32),
        grid_spec=pltpu.PrefetchScalarGridSpec(
            num_scalar_prefetch=1, grid=(n_tiles,),
            in_specs=[pl.BlockSpec((n_tok, d_model), lambda j, b: (0, 0)),
                      pl.BlockSpec((2, n_tok), lambda j, b: (0, 0)),
                      pl.BlockSpec((1, n_tok), lambda j, b: (0, 0)), rows, rows] + [pl.BlockSpec(memory_space=pl.ANY)] * (held is not None),
            out_specs=pl.BlockSpec((TILE, d_model), lambda j, b: (first + j, 0)),
            scratch_shapes=[pltpu.VMEM((TILE, d_model), jnp.float32)]),
        input_output_aliases={} if held is None else {6: 0},
        compiler_params=params(),
        cost_estimate=pl.CostEstimate(flops=4 * n_tiles * TILE * n_tok * d_model, bytes_accessed=n_tiles * TILE * d_model * 12, transcendentals=0),
        name='head_rows',
    )(blocks + first, z_all, norm, targets, embed_table, grad_embed, *([] if held is None else [held]))


def head_grads(z_all, norm, targets, embed_table, grad_embed, blocks, n_own, n_tiles, n_rep, with_top):
    vocab, d_model = embed_table.shape
    n_tok = z_all.shape[0]
    n_chunks = n_tok // CHUNK
    last = (vocab - 1) // TILE
    out_shape = [jax.ShapeDtypeStruct((n_own * TILE, d_model), jnp.float32)]
    out_specs = [pl.BlockSpec((TILE, d_model), lambda j, b: (jnp.minimum(j, n_own - 1), 0))]
    if with_top:
        out_shape.append(jax.ShapeDtypeStruct((n_chunks, CHUNK, d_model), jnp.float32))
        out_specs.append(pl.BlockSpec((n_chunks, CHUNK, d_model), lambda j, b: (0, 0, 0), pipeline_mode=pl.Buffered(1)))
    return pl.pallas_call(
        functools.partial(head_kernel, vocab, n_chunks, n_rep, n_own, with_top),
        out_shape=out_shape,
        grid_spec=pltpu.PrefetchScalarGridSpec(
            num_scalar_prefetch=1, grid=(n_tiles,),
            in_specs=[pl.BlockSpec((n_tok, d_model), lambda j, b: (0, 0)),
                      pl.BlockSpec((2, n_tok), lambda j, b: (0, 0)),
                      pl.BlockSpec((1, n_tok), lambda j, b: (0, 0)),
                      pl.BlockSpec((TILE, d_model), lambda j, b: (jnp.minimum(tile_of(n_own, b, j), last), 0)),
                      pl.BlockSpec((TILE, d_model), lambda j, b: (jnp.minimum(b[0] + jnp.minimum(j, n_own - 1), last), 0))],
            out_specs=out_specs,
            scratch_shapes=[pltpu.VMEM((n_chunks, d_model, CHUNK), jnp.float32)] * with_top + [pltpu.VMEM((TILE, d_model), jnp.float32)]),
        compiler_params=params(),
        cost_estimate=pl.CostEstimate(flops=(6 if with_top else 4) * n_tiles * TILE * n_tok * d_model,
                                      bytes_accessed=n_tiles * TILE * d_model * 12, transcendentals=0),
        name='head_grads' if with_top else 'head_rows',
    )(blocks, z_all, norm, targets, embed_table, grad_embed)


def sparse_rows(block, start_ref, ids_ref, low_ref, base):
    rows = block * TILE + lax.broadcasted_iota(jnp.int32, (TILE, 1), 0)
    first = start_ref[block] // SEG
    stop = (start_ref[block + 1] + SEG - 1) // SEG

    def segment(c, acc):
        pick = jnp.where(rows == ids_ref[pl.ds(c, 1), :], 1.0, 0.0).astype(jnp.bfloat16)
        return acc + jnp.dot(pick, low_ref[pl.ds(pl.multiple_of(c * SEG, SEG), SEG), :], preferred_element_type=jnp.float32)

    return lax.fori_loop(first, stop, segment, base)


def sumsq_kernel(low_scale, blk_ref, start_ref, ids_ref, low_ref, g_ref, out_ref):
    block = blk_ref[0] + pl.program_id(0)
    zero = jnp.zeros(g_ref.shape, jnp.float32)
    full = g_ref[...] + low_scale * sparse_rows(block, start_ref, ids_ref, low_ref, zero)

    @pl.when(pl.program_id(0) == 0)
    def _():
        out_ref[...] = jnp.zeros_like(out_ref)

    out_ref[...] += jnp.sum((full * full).reshape(-1, 8, full.shape[1]), axis=0)


def rows_sumsq(blocks, starts, ids, low, g_rows, n_tiles, low_scale):
    d_model = g_rows.shape[1]
    return pl.pallas_call(
        functools.partial(sumsq_kernel, low_scale),
        out_shape=jax.ShapeDtypeStruct((8, d_model), jnp.float32),
        grid_spec=pltpu.PrefetchScalarGridSpec(
            num_scalar_prefetch=2, grid=(n_tiles,),
            in_specs=[pl.BlockSpec(ids.shape, lambda j, b, s: (0, 0)),
                      pl.BlockSpec(low.shape, lambda j, b, s: (0, 0)),
                      pl.BlockSpec((TILE, d_model), lambda j, b, s: (b[1] + j, 0))],
            out_specs=pl.BlockSpec((8, d_model), lambda j, b, s: (0, 0))),
        compiler_params=params(),
        name='rows_sumsq',
    )(blocks, starts, ids, low, g_rows)


def adam_kernel(low_scale, n_wide, n_red, start_ref, stage_ref, clip_ref, ids_ref, low_ref, gw_ref, go_ref, gf_ref,
                w_ref, m_ref, v_ref, w_out, m_out, v_out, acc_ref):
    j = pl.program_id(0)
    own = n_wide + n_red * stage_ref[0]
    is_own = (j >= own) & (j < own + n_red)

    rows = j * ADAM_TILE + lax.broadcasted_iota(jnp.int32, (ADAM_TILE, 1), 0)
    per = ADAM_TILE // TILE
    first = jnp.minimum(start_ref[per * j] // SEG, ids_ref.shape[0] - 1)

    def segment(c):
        pick = jnp.where(rows == ids_ref[pl.ds(c, 1), :], 1.0, 0.0).astype(jnp.bfloat16)
        return low_scale * jnp.dot(pick, low_ref[pl.ds(pl.multiple_of(c * SEG, SEG), SEG), :], preferred_element_type=jnp.float32)

    @pl.when(j < n_wide)
    def _():
        acc_ref[...] = gw_ref[...] + segment(first)

    @pl.when(is_own)
    def _():
        acc_ref[...] = go_ref[...] + segment(first)

    @pl.when((j >= n_wide) & jnp.logical_not(is_own))
    def _():
        acc_ref[...] = gf_ref[...] + segment(first)

    def add(c, _):
        acc_ref[...] += segment(c)
        return 0

    lax.fori_loop(first + 1, (start_ref[per * j + per] + SEG - 1) // SEG, add, 0)

    def part(i, _):
        r = pl.ds(pl.multiple_of(i * 32, 32), 32)
        w_new, m_new, v_new = adamw_update(w_ref[r, :], m_ref[r, :], v_ref[r, :], acc_ref[r, :], clip_ref[0])
        w_out[r, :] = w_new
        m_out[r, :] = m_new
        v_out[r, :] = v_new
        return 0

    lax.fori_loop(0, ADAM_TILE // 32, part, 0)


def embed_adam(starts, stage, clip, ids, low, g_wide, g_own, g_far, embed_table, mom, vel, low_scale):
    vocab, d_model = embed_table.shape
    n_wide, n_red = g_wide.shape[0] // ADAM_TILE, g_own.shape[0] // ADAM_TILE
    spec = pl.BlockSpec((ADAM_TILE, d_model), lambda j, s, t, c: (j, 0))
    shape = jax.ShapeDtypeStruct((vocab, d_model), jnp.float32)

    def held(first):
        return pl.BlockSpec((ADAM_TILE, d_model), lambda j, s, t, c: (jnp.clip(j - n_wide - n_red * first(t[0]), 0, n_red - 1), 0))

    return pl.pallas_call(
        functools.partial(adam_kernel, low_scale, n_wide, n_red),
        out_shape=[shape] * 3,
        grid_spec=pltpu.PrefetchScalarGridSpec(
            num_scalar_prefetch=3, grid=(pl.cdiv(vocab, ADAM_TILE),),
            in_specs=[pl.BlockSpec(ids.shape, lambda j, s, t, c: (0, 0)),
                      pl.BlockSpec(low.shape, lambda j, s, t, c: (0, 0)),
                      pl.BlockSpec((ADAM_TILE, d_model), lambda j, s, t, c: (jnp.minimum(j, n_wide - 1), 0)),
                      held(lambda t: t), held(lambda t: 1 - t), spec, spec, spec],
            out_specs=[spec] * 3,
            scratch_shapes=[pltpu.VMEM((ADAM_TILE, d_model), jnp.float32)]),
        compiler_params=params(),
        cost_estimate=pl.CostEstimate(flops=20 * vocab * d_model, bytes_accessed=28 * vocab * d_model, transcendentals=0),
        name='embed_adam',
    )(starts, stage, clip, ids, low, g_wide, g_own, g_far, embed_table, mom, vel)


def next_kernel(scale, n_blocks, ids_ref, table_ref, wi0_ref, wo0_ref, wi1_ref, wo1_ref, out_ref, rows_ref, x_ref, acc_ref, sems):
    blk = pl.program_id(0)
    slot = lax.rem(blk, 2)
    n_ff = wi0_ref.shape[1] // FWD_CHUNK
    per = TOKEN_BLOCK // (2 * n_ff)

    def fetch(base, to_slot, first, count):
        for t in range(count):
            row = ids_ref[base + first + t]
            pltpu.make_async_copy(table_ref.at[pl.ds(row, 1), :], rows_ref.at[to_slot, pl.ds(first + t, 1), :], sems.at[to_slot]).start()

    @pl.when(blk == 0)
    def _():
        def step(i, _):
            fetch(0, 0, i * 16, 16)
            return 0
        lax.fori_loop(0, TOKEN_BLOCK // 16, step, 0)

    pltpu.make_async_copy(rows_ref.at[1 - slot], rows_ref.at[slot], sems.at[slot]).wait()
    base = jnp.minimum(blk + 1, n_blocks - 1) * TOKEN_BLOCK
    x_ref[...] = (scale * rows_ref[slot].astype(jnp.bfloat16).astype(jnp.float32)).astype(jnp.bfloat16)

    for layer, (wi_ref, wo_ref) in enumerate(((wi0_ref, wo0_ref), (wi1_ref, wo1_ref))):
        acc_ref[...] = x_ref[...].astype(jnp.float32)
        for c in range(n_ff):
            fetch(base, 1 - slot, (layer * n_ff + c) * per, per)
            cols = pl.ds(c * FWD_CHUNK, FWD_CHUNK)
            pre_act = jnp.dot(x_ref[...], wi_ref[:, cols], preferred_element_type=jnp.float32)
            bend = jnp.tanh(pre_act * (GELU_K + (GELU_K * GELU_A) * (pre_act * pre_act)))
            hidden = ((0.5 * pre_act) * (1.0 + bend)).astype(jnp.bfloat16)
            acc_ref[...] += jnp.dot(hidden, wo_ref[cols, :], preferred_element_type=jnp.float32)
        if layer == 0:
            x_ref[...] = acc_ref[...].astype(jnp.bfloat16)
        else:
            out_ref[...] = acc_ref[...].astype(jnp.bfloat16)

    @pl.when(blk == n_blocks - 1)
    def _():
        pltpu.make_async_copy(rows_ref.at[slot], rows_ref.at[1 - slot], sems.at[1 - slot]).wait()


def next_forward(ids, table, wi0, wo0, wi1, wo1, scale):
    n_tok = ids.shape[0]
    d_model = table.shape[1]
    whole = [pl.BlockSpec(w.shape, lambda j, s: (0, 0)) for w in (wi0, wo0, wi1, wo1)]
    return pl.pallas_call(
        functools.partial(next_kernel, scale, n_tok // TOKEN_BLOCK),
        out_shape=jax.ShapeDtypeStruct((n_tok, d_model), jnp.bfloat16),
        grid_spec=pltpu.PrefetchScalarGridSpec(
            num_scalar_prefetch=1, grid=(n_tok // TOKEN_BLOCK,),
            in_specs=[pl.BlockSpec(memory_space=pl.ANY)] + whole,
            out_specs=pl.BlockSpec((TOKEN_BLOCK, d_model), lambda j, s: (j, 0)),
            scratch_shapes=[pltpu.VMEM((2, TOKEN_BLOCK, d_model), jnp.float32), pltpu.VMEM((TOKEN_BLOCK, d_model), jnp.bfloat16),
                            pltpu.VMEM((TOKEN_BLOCK, d_model), jnp.float32), pltpu.SemaphoreType.DMA((2,))]),
        compiler_params=params(),
        cost_estimate=pl.CostEstimate(flops=8 * n_tok * d_model * wi0.shape[1], bytes_accessed=6 * n_tok * d_model, transcendentals=0),
        name='next_forward',
    )(ids, table, wi0, wo0, wi1, wo1)


def exchange(x_ref, all_ref, send_sems, recv_sems):
    n_stage = lax.axis_size('stage')
    me = lax.axis_index('data') * n_stage + lax.axis_index('stage')

    def place(k):
        to = lax.rem(me + k, N_DEV)
        return to // n_stage, lax.rem(to, n_stage)

    barrier = pltpu.get_barrier_semaphore()
    for k in range(1, N_DEV):
        pl.semaphore_signal(barrier, inc=1, device_id=place(k), device_id_type=MESH_ID)
    pl.semaphore_wait(barrier, N_DEV - 1)
    copies = []
    for k in range(1, N_DEV):
        copies.append(pltpu.make_async_remote_copy(
            src_ref=x_ref, dst_ref=all_ref.at[k - 1], send_sem=send_sems.at[k - 1], recv_sem=recv_sems.at[k - 1],
            device_id=place(k), device_id_type=MESH_ID))
        copies[-1].start()
    for copy in copies:
        copy.wait()


def norm_kernel(x_ref, out_ref, all_ref, send_sems, recv_sems):
    exchange(x_ref, all_ref, send_sems, recv_sems)
    top = x_ref[0:1, :]
    for k in range(N_DEV - 1):
        top = jnp.maximum(top, all_ref[k, 0:1, :])
    total = x_ref[1:2, :] * jnp.exp(x_ref[0:1, :] - top)
    for k in range(N_DEV - 1):
        total += all_ref[k, 1:2, :] * jnp.exp(all_ref[k, 0:1, :] - top)
    out_ref[0:1, :] = top
    out_ref[1:2, :] = 1.0 / total


def gather_kernel(x_ref, out_ref, all_ref, send_sems, recv_sems):
    exchange(x_ref, all_ref, send_sems, recv_sems)
    me = lax.axis_index('data') * lax.axis_size('stage') + lax.axis_index('stage')
    out_ref[pl.ds(me, 1)] = x_ref[...][None]
    for k in range(N_DEV - 1):
        out_ref[pl.ds(lax.rem(me + (N_DEV - 1 - k), N_DEV), 1)] = all_ref[k:k + 1]


def small_exchange(body, x, out_shape, collective_id, name):
    return pl.pallas_call(
        body,
        out_shape=out_shape,
        in_specs=[pl.BlockSpec(memory_space=pltpu.VMEM)],
        out_specs=pl.BlockSpec(memory_space=pltpu.VMEM),
        scratch_shapes=[pltpu.VMEM((N_DEV - 1,) + x.shape, x.dtype), pltpu.SemaphoreType.DMA((N_DEV - 1,)),
                        pltpu.SemaphoreType.DMA((N_DEV - 1,))],
        compiler_params=pltpu.CompilerParams(collective_id=collective_id, has_side_effects=True),
        name=name,
    )(x)


def solution(mesh):
    n_stage = mesh.shape['stage']
    n_rep = mesh.shape['data']
    n_dev = n_stage * n_rep
    swap = [(0, 1), (1, 0)]
    w_spec = P('stage', None, None)
    in_specs = (w_spec,) * 8 + (P(None, None),) * 4 + (P('stage', 'data', None), P('data'), P('data'), P(None, 'data'), P(None))
    out_specs = (w_spec,) * 6 + (P(None, None),) * 3 + (P(None, 'data', None),)

    def local_step(w_first, w_second, mom_first, mom_second, vel_first, vel_second, grad_first, grad_second,
                   embed_table, mom_embed, vel_embed, grad_embed, stage_acts, last_tokens, targets, next_tokens, max_norm):
        stage_id = lax.axis_index('stage')
        dev_id = lax.axis_index('data') * n_stage + stage_id
        low_core = stage_id == 0
        vocab, d_model = embed_table.shape
        scale_in = math.sqrt(d_model)
        low_scale = scale_in / n_rep
        n_tiles = -(-vocab // (TILE * n_dev))
        n_wide = WIDE_TILES
        n_rest = n_tiles - n_wide
        n_red = n_rest * n_dev // n_stage
        n_part = n_red // n_rep
        rest0 = n_dev * n_wide

        def other(x):
            return lax.ppermute(x, 'stage', swap)

        def by_stage(own, far):
            return jnp.where(low_core, own, far), jnp.where(low_core, far, own)

        w_in, w_out = w_first[0].astype(jnp.bfloat16), w_second[0].astype(jnp.bfloat16)
        w_in0, w_in1 = by_stage(w_in, other(w_in))
        w_out0, w_out1 = by_stage(w_out, other(w_out))

        z_own = block_forward(stage_acts[0], w_in, w_out)
        cut = z_own.shape[0] // 2
        z_piece = jnp.where(low_core, lax.ppermute(z_own[:cut], 'stage', [(1, 0)]), z_own[cut:])
        all_ids = lax.all_gather(jnp.stack([last_tokens, targets]), 'data', axis=1, tiled=True)
        ids, tgts = all_ids[0], all_ids[1:2]
        n_tok = ids.shape[0]
        half = n_tok // 2
        z_all = lax.all_gather(z_piece, BOTH, axis=0, tiled=True)

        order = jnp.arange(n_tok, dtype=jnp.int32)
        before = (ids[None, :] < ids[:, None]) | ((ids[None, :] == ids[:, None]) & (order[None, :] < order[:, None]))
        rank = jnp.sum(before.astype(jnp.int32), axis=1)
        edges = TILE * jnp.arange(n_tiles * n_dev + 1, dtype=jnp.int32)
        starts = jnp.sum((ids[None, :] < edges[:, None]).astype(jnp.int32), axis=1)
        z_all, rank, starts, acts_in = lax.optimization_barrier((z_all, rank, starts, stage_acts[0]))

        acts = lax.all_gather(acts_in, 'data', axis=0, tiled=True)

        def blocks(*tiles):
            return jnp.stack([jnp.asarray(t, jnp.int32) for t in tiles])

        shard = blocks(dev_id * n_wide, rest0 + dev_id * n_rest - n_wide)
        stat = head_stats(z_all, embed_table, shard, n_wide, n_tiles)
        norm = small_exchange(norm_kernel, stat, jax.ShapeDtypeStruct(stat.shape, jnp.float32), 1, 'share_stats')
        norm, acts = lax.optimization_barrier((norm, acts))
        mine = lax.dynamic_slice_in_dim(acts, stage_id * half, half)
        far = other(lax.dynamic_slice_in_dim(acts, (1 - stage_id) * half, half))
        act0, act1 = by_stage(mine, far)
        g_shard, d_top_part = head_grads(z_all, norm, tgts, embed_table, grad_embed, shard, n_wide, n_tiles, n_rep, True)
        d_top_own = lax.psum_scatter(d_top_part, BOTH, scatter_dimension=0, tiled=True)
        red_tile = rest0 + stage_id * n_red
        red = blocks(red_tile, red_tile)
        n_early = n_red - n_red // 4
        g_own = head_rows(z_all, norm, tgts, embed_table, grad_embed, red, n_red, 0, n_early, n_rep)
        d_top_own, g_own = lax.optimization_barrier((d_top_own, g_own))
        d_top_own = d_top_own.reshape(-1, d_model).astype(jnp.bfloat16)
        g_shard, d_top_own, late_ids = lax.optimization_barrier((g_shard, d_top_own, ids))
        d_top = lax.all_gather(d_top_own, BOTH, axis=0, tiled=True)
        sorted_ids = jnp.sum(jnp.where(rank[None, :] == order[:, None], late_ids[None, :], 0), axis=1).reshape(n_tok // SEG, SEG)
        g_own = head_rows(z_all, norm, tgts, embed_table, grad_embed, red, n_red, n_early, n_red - n_early, n_rep, g_own)
        d_top, sorted_ids, g_own = lax.optimization_barrier((d_top, sorted_ids, g_own))
        g_far = other(g_own)
        g_wide = lax.all_gather(g_shard, BOTH, axis=0, tiled=True)

        d_half = lax.dynamic_slice_in_dim(d_top, stage_id * half, half)
        olds = (grad_first[0], grad_second[0], n_rep)
        d_act1, full_in1, full_out1, sq1 = block_backward(d_half, act1, w_in1, w_out1, *olds, 3)
        d_low_half, full_in0, full_out0, sq0 = block_backward(d_act1, act0, w_in0, w_out0, *olds, 4)
        my_rank = lax.dynamic_slice_in_dim(rank, stage_id * half, half)
        perm = (my_rank[None, :] == order[:, None]).astype(jnp.bfloat16)
        low_half = jnp.dot(perm, d_low_half, preferred_element_type=jnp.float32).astype(jnp.bfloat16)
        low = low_half + other(low_half)

        full_first = jnp.where(low_core, full_in0, full_in1)
        full_second = jnp.where(low_core, full_out0, full_out1)

        my_part = lax.axis_index('data') * n_part
        embed_sq = (jnp.sum(rows_sumsq(blocks(dev_id * n_wide, 0), starts, sorted_ids, low, g_shard, n_wide, low_scale))
                    + jnp.sum(rows_sumsq(blocks(red_tile + my_part, my_part), starts, sorted_ids, low, g_own, n_part, low_scale)))
        stage_sq = jnp.sum(jnp.where(low_core, sq0, sq1))
        own_sq = jnp.full((8, 128), embed_sq + stage_sq / n_rep)
        all_sq = small_exchange(gather_kernel, own_sq, jax.ShapeDtypeStruct((n_dev, 8, 128), jnp.float32), 2, 'share_sums')
        total_sq = jnp.sum(all_sq[:, 0, 0])
        clip_scale = jnp.minimum(1.0, max_norm[0] / (jnp.sqrt(total_sq) + CLIP_EPS))
        new_first, new_mom_first, new_vel_first = adamw_update(w_first[0], mom_first[0], vel_first[0], full_first, clip_scale)
        new_second, new_mom_second, new_vel_second = adamw_update(w_second[0], mom_second[0], vel_second[0], full_second, clip_scale)
        new_embed, new_mom_embed, new_vel_embed = embed_adam(
            starts, blocks(stage_id), clip_scale.reshape(1), sorted_ids, low, g_wide, g_own, g_far, embed_table, mom_embed, vel_embed, low_scale)

        next_in, next_out = new_first.astype(jnp.bfloat16), new_second.astype(jnp.bfloat16)
        next_in0, next_in1 = by_stage(next_in, other(next_in))
        next_out0, next_out1 = by_stage(next_out, other(next_out))
        n_micro, tokens = next_tokens.shape
        my_micro = n_micro // n_stage
        my_rows = lax.dynamic_slice_in_dim(next_tokens, stage_id * my_micro, my_micro).reshape(2, -1)
        gathered = []
        for piece in range(2):
            final_act = next_forward(my_rows[piece], new_embed, next_in0, next_out0, next_in1, next_out1, scale_in)
            gathered.append(lax.all_gather(final_act.reshape(my_micro // 2, tokens, d_model), 'stage', axis=0, tiled=False))
        next_acts = jnp.stack(gathered, axis=1).reshape(n_micro, tokens, d_model)
        return (new_first[None], new_second[None], new_mom_first[None], new_mom_second[None],
                new_vel_first[None], new_vel_second[None], new_embed, new_mom_embed, new_vel_embed, next_acts)

    return jax.shard_map(local_step, mesh=mesh, in_specs=in_specs, out_specs=out_specs, check_vma=False)
```

```python
import functools
import math
import jax
import jax.numpy as jnp
from jax import lax
from jax.experimental import pallas as pl
from jax.experimental.pallas import tpu as pltpu
from jax.sharding import PartitionSpec as P

STEP_COUNT = 10
LEARN_RATE = 1e-3
ADAM_BETA1 = 0.9
ADAM_BETA2 = 0.95
ADAM_EPS = 1e-8
WEIGHT_DECAY = 0.1
CLIP_EPS = 1e-6

TILE = 512
ADAM_TILE = 1024
CHUNK = 512
SEG = 256
TOKEN_BLOCK = 512
FF_CHUNK = 512
FWD_CHUNK = 1024
N_DEV = 8
MESH_ID = pl.DeviceIdType.MESH
WIDE_TILES = 5
NEG = -1e30
GELU_K = math.sqrt(2.0 / math.pi)
GELU_A = 0.044715
BOTH = ('data', 'stage')


def block_forward(act_in, w_in, w_out):
    pre_act = jnp.dot(act_in, w_in, preferred_element_type=jnp.float32)
    hidden = jax.nn.gelu(pre_act).astype(jnp.bfloat16)
    mlp_out = jnp.dot(hidden, w_out, preferred_element_type=jnp.float32)
    return (act_in.astype(jnp.float32) + mlp_out).astype(jnp.bfloat16)


def backward_kernel(n_chunks, n_ff, n_rep, g_ref, x_ref, wi_ref, wo_ref, old_i_ref, old_o_ref, dx_ref, full_i_ref, full_o_ref, sq_ref,
                    back_ref, part_ref, far_ref, send_sems, recv_sems):
    f = pl.program_id(0)
    partner = (lax.axis_index('data'), 1 - lax.axis_index('stage'))

    def copy(i, which):
        return pltpu.make_async_remote_copy(
            src_ref=part_ref.at[i, which], dst_ref=far_ref.at[i, which], send_sem=send_sems.at[i, which],
            recv_sem=recv_sems.at[i, which], device_id=partner, device_id_type=MESH_ID)

    @pl.when(f == 0)
    def _():
        barrier = pltpu.get_barrier_semaphore()
        pl.semaphore_signal(barrier, inc=1, device_id=partner, device_id_type=MESH_ID)
        pl.semaphore_wait(barrier, 1)
        back_ref[...] = jnp.zeros_like(back_ref)

    for i in range(n_ff - 1):
        @pl.when(f == i + 1)
        def _():
            copy(i, 0).start()
            copy(i, 1).start()

    wi = wi_ref[...]
    wi_flip = wi.T
    part_ref[f] = jnp.zeros(part_ref.shape[1:], jnp.float32)

    def chunk(c, _):
        rows = pl.ds(pl.multiple_of(c * CHUNK, CHUNK), CHUNK)
        x, g = x_ref[rows, :], g_ref[rows, :]
        pre = dot_last(wi_flip, x)
        d_hidden = dot_last(wo_ref[...], g)
        square = pre * pre
        bend = jnp.tanh(GELU_K * pre * (1.0 + GELU_A * square))
        rise = 0.5 * (1.0 + bend)
        hidden = (pre * rise).astype(jnp.bfloat16)
        slope = rise + (0.5 * GELU_K) * pre * (1.0 - bend * bend) * (1.0 + (3.0 * GELU_A) * square)
        d_pre = (d_hidden * slope).astype(jnp.bfloat16)
        part_ref[f, 0] += jnp.dot(d_pre, x, preferred_element_type=jnp.float32)
        part_ref[f, 1] += jnp.dot(hidden, g, preferred_element_type=jnp.float32)
        back_ref[c] += jnp.dot(wi, d_pre, preferred_element_type=jnp.float32)
        return 0

    lax.fori_loop(0, n_chunks, chunk, 0, unroll=2)

    @pl.when(f == n_ff - 1)
    def _():
        sq_ref[...] = jnp.zeros_like(sq_ref)

        def last(c, _):
            rows = pl.ds(pl.multiple_of(c * CHUNK, CHUNK), CHUNK)
            dx_ref[rows, :] = (g_ref[rows, :].astype(jnp.float32) + back_ref[c].T).astype(jnp.bfloat16)
            return 0

        def squares(x):
            sq_ref[...] += jnp.sum((x * x).reshape(-1, 8, x.shape[1]), axis=0)

        lax.fori_loop(0, n_chunks, last, 0)
        copy(n_ff - 1, 0).start()
        copy(n_ff - 1, 1).start()
        for i in range(n_ff):
            part = pl.ds(i * FF_CHUNK, FF_CHUNK)
            copy(i, 0).wait()
            copy(i, 1).wait()
            full_i = old_i_ref[:, part] + (part_ref[i, 0] + far_ref[i, 0]).T * (1.0 / n_rep)
            full_i_ref[:, part] = full_i
            squares(full_i)
            full_o = old_o_ref[part, :] + (part_ref[i, 1] + far_ref[i, 1]) * (1.0 / n_rep)
            full_o_ref[part, :] = full_o
            squares(full_o)


def block_backward(d_out, act_in, w_in, w_out, old_in, old_out, n_rep, collective_id):
    n_tok, d_model = act_in.shape
    ff = w_in.shape[1]
    n_chunks, n_ff = n_tok // CHUNK, ff // FF_CHUNK

    def whole(*shape):
        return pl.BlockSpec(shape, lambda f: (0, 0), pipeline_mode=pl.Buffered(1))

    tokens = whole(n_tok, d_model)
    part = (n_ff, 2, FF_CHUNK, d_model)
    return pl.pallas_call(
        functools.partial(backward_kernel, n_chunks, n_ff, n_rep),
        out_shape=[jax.ShapeDtypeStruct((n_tok, d_model), jnp.bfloat16), jax.ShapeDtypeStruct((d_model, ff), jnp.float32),
                   jax.ShapeDtypeStruct((ff, d_model), jnp.float32), jax.ShapeDtypeStruct((8, d_model), jnp.float32)],
        grid=(n_ff,),
        in_specs=[tokens, tokens, pl.BlockSpec((d_model, FF_CHUNK), lambda f: (0, f)), pl.BlockSpec((FF_CHUNK, d_model), lambda f: (f, 0)),
                  whole(d_model, ff), whole(ff, d_model)],
        out_specs=[tokens, whole(d_model, ff), whole(ff, d_model), whole(8, d_model)],
        scratch_shapes=[pltpu.VMEM((n_chunks, d_model, CHUNK), jnp.float32), pltpu.VMEM(part, jnp.float32), pltpu.VMEM(part, jnp.float32),
                        pltpu.SemaphoreType.DMA((n_ff, 2)), pltpu.SemaphoreType.DMA((n_ff, 2))],
        compiler_params=params(collective_id=collective_id, has_side_effects=True),
        cost_estimate=pl.CostEstimate(flops=10 * n_tok * d_model * ff, bytes_accessed=12 * d_model * ff, transcendentals=0),
        name='block_backward',
    )(d_out, act_in, w_in, w_out, old_in, old_out)


def adamw_update(master, moment, velocity, gradient, clip_scale):
    scaled_grad = clip_scale * gradient
    moment_new = ADAM_BETA1 * moment + (1.0 - ADAM_BETA1) * scaled_grad
    velocity_new = ADAM_BETA2 * velocity + (1.0 - ADAM_BETA2) * scaled_grad * scaled_grad
    moment_hat = moment_new / (1.0 - ADAM_BETA1 ** STEP_COUNT)
    velocity_hat = velocity_new / (1.0 - ADAM_BETA2 ** STEP_COUNT)
    master_new = master - LEARN_RATE * (moment_hat / (jnp.sqrt(velocity_hat) + ADAM_EPS) + WEIGHT_DECAY * master)
    return master_new, moment_new, velocity_new


def dot_last(a, b):
    return lax.dot_general(a, b, (((1,), (1,)), ((), ())), preferred_element_type=jnp.float32)


def params(limit_mib=60, **kw):
    return pltpu.CompilerParams(vmem_limit_bytes=limit_mib * 1024 * 1024, **kw)


def load_rows(block, e_ref, vocab):
    rows = block * TILE + lax.broadcasted_iota(jnp.int32, (TILE, 1), 0)
    valid = rows < vocab
    e_tile = jnp.where(valid, e_ref[...], 0.0).astype(jnp.bfloat16)
    return rows, valid, e_tile, jnp.where(valid, 0.0, NEG)


def tile_of(n_own, blk_ref, j):
    return jnp.where(j < n_own, blk_ref[0] + j, blk_ref[1] + j)


def stats_kernel(vocab, n_chunks, n_own, blk_ref, z_ref, e_ref, stat_ref):
    _, _, e_tile, bias = load_rows(tile_of(n_own, blk_ref, pl.program_id(0)), e_ref, vocab)

    @pl.when(pl.program_id(0) == 0)
    def _():
        stat_ref[0:1, :] = jnp.full((1, stat_ref.shape[1]), NEG, jnp.float32)
        stat_ref[1:2, :] = jnp.zeros((1, stat_ref.shape[1]), jnp.float32)

    def chunk(c, _):
        cols = pl.ds(pl.multiple_of(c * CHUNK, CHUNK), CHUNK)
        logits = dot_last(e_tile, z_ref[cols, :]) + bias
        top_old = stat_ref[0:1, cols]
        top_new = jnp.maximum(top_old, jnp.max(logits, axis=0, keepdims=True))
        part = jnp.sum(jnp.exp(logits - top_new), axis=0, keepdims=True)
        stat_ref[0:1, cols] = top_new
        stat_ref[1:2, cols] = stat_ref[1:2, cols] * jnp.exp(top_old - top_new) + part
        return 0

    lax.fori_loop(0, n_chunks, chunk, 0, unroll=4)


def head_stats(z_all, embed_table, blocks, n_own, n_tiles):
    vocab, d_model = embed_table.shape
    n_tok = z_all.shape[0]
    last = (vocab - 1) // TILE
    return pl.pallas_call(
        functools.partial(stats_kernel, vocab, n_tok // CHUNK, n_own),
        out_shape=jax.ShapeDtypeStruct((2, n_tok), jnp.float32),
        grid_spec=pltpu.PrefetchScalarGridSpec(
            num_scalar_prefetch=1, grid=(n_tiles,),
            in_specs=[pl.BlockSpec((n_tok, d_model), lambda j, b: (0, 0)),
                      pl.BlockSpec((TILE, d_model), lambda j, b: (jnp.minimum(tile_of(n_own, b, j), last), 0))],
            out_specs=pl.BlockSpec((2, n_tok), lambda j, b: (0, 0))),
        compiler_params=params(),
        cost_estimate=pl.CostEstimate(flops=2 * n_tiles * TILE * n_tok * d_model, bytes_accessed=n_tiles * TILE * d_model * 4, transcendentals=0),
        name='head_stats',
    )(blocks, z_all, embed_table)


def head_kernel(vocab, n_chunks, n_rep, n_own, with_top, blk_ref, z_ref, norm_ref, tgt_ref, e_ref, g_ref, out_ref, *rest):
    top_ref = rest[1] if with_top else None
    acc_ref = rest[-1]
    j = pl.program_id(0)
    rows, valid, e_tile, bias = load_rows(tile_of(n_own, blk_ref, j), e_ref, vocab)
    if with_top:
        e_flip = e_tile.T

        @pl.when(j == 0)
        def _():
            top_ref[...] = jnp.zeros_like(top_ref)

    def chunk(with_rows, c, _):
        cols = pl.ds(pl.multiple_of(c * CHUNK, CHUNK), CHUNK)
        z_chunk = z_ref[cols, :]
        logits = dot_last(e_tile, z_chunk) + bias
        probs = jnp.exp(logits - norm_ref[0:1, cols]) * norm_ref[1:2, cols]
        d_logits = jnp.where(rows == tgt_ref[0:1, cols], probs - 1.0, probs).astype(jnp.bfloat16)
        if with_rows:
            acc_ref[...] += jnp.dot(d_logits, z_chunk, preferred_element_type=jnp.float32)
        if with_top:
            top_ref[c] += jnp.dot(e_flip, d_logits, preferred_element_type=jnp.float32)
        return 0

    @pl.when(j < n_own)
    def _():
        acc_ref[...] = jnp.zeros_like(acc_ref)
        lax.fori_loop(0, n_chunks, functools.partial(chunk, True), 0, unroll=2 if with_top else 4)
        out_ref[...] = jnp.where(valid, g_ref[...], 0.0) + acc_ref[...] * (1.0 / n_rep)

    if with_top:
        @pl.when(j >= n_own)
        def _():
            lax.fori_loop(0, n_chunks, functools.partial(chunk, False), 0, unroll=2)

        @pl.when(j == pl.num_programs(0) - 1)
        def _():
            def turn(c, _):
                rest[0][c] = top_ref[c].T
                return 0
            lax.fori_loop(0, n_chunks, turn, 0)


def head_rows(z_all, norm, targets, embed_table, grad_embed, blocks, n_own, first, n_tiles, n_rep, held=None):
    vocab, d_model = embed_table.shape
    n_tok = z_all.shape[0]
    last = (vocab - 1) // TILE
    rows = pl.BlockSpec((TILE, d_model), lambda j, b: (jnp.minimum(b[0] + j, last), 0))

    def kernel(blk_ref, z_ref, norm_ref, tgt_ref, e_ref, g_ref, *rest):
        head_kernel(vocab, n_tok // CHUNK, n_rep, n_own, False, blk_ref, z_ref, norm_ref, tgt_ref, e_ref, g_ref, *rest[-2:])

    return pl.pallas_call(
        kernel,
        out_shape=jax.ShapeDtypeStruct((n_own * TILE, d_model), jnp.float32),
        grid_spec=pltpu.PrefetchScalarGridSpec(
            num_scalar_prefetch=1, grid=(n_tiles,),
            in_specs=[pl.BlockSpec((n_tok, d_model), lambda j, b: (0, 0)),
                      pl.BlockSpec((2, n_tok), lambda j, b: (0, 0)),
                      pl.BlockSpec((1, n_tok), lambda j, b: (0, 0)), rows, rows] + [pl.BlockSpec(memory_space=pl.ANY)] * (held is not None),
            out_specs=pl.BlockSpec((TILE, d_model), lambda j, b: (first + j, 0)),
            scratch_shapes=[pltpu.VMEM((TILE, d_model), jnp.float32)]),
        input_output_aliases={} if held is None else {6: 0},
        compiler_params=params(),
        cost_estimate=pl.CostEstimate(flops=4 * n_tiles * TILE * n_tok * d_model, bytes_accessed=n_tiles * TILE * d_model * 12, transcendentals=0),
        name='head_rows',
    )(blocks + first, z_all, norm, targets, embed_table, grad_embed, *([] if held is None else [held]))


def head_grads(z_all, norm, targets, embed_table, grad_embed, blocks, n_own, n_tiles, n_rep, with_top):
    vocab, d_model = embed_table.shape
    n_tok = z_all.shape[0]
    n_chunks = n_tok // CHUNK
    last = (vocab - 1) // TILE
    out_shape = [jax.ShapeDtypeStruct((n_own * TILE, d_model), jnp.float32)]
    out_specs = [pl.BlockSpec((TILE, d_model), lambda j, b: (jnp.minimum(j, n_own - 1), 0))]
    if with_top:
        out_shape.append(jax.ShapeDtypeStruct((n_chunks, CHUNK, d_model), jnp.float32))
        out_specs.append(pl.BlockSpec((n_chunks, CHUNK, d_model), lambda j, b: (0, 0, 0), pipeline_mode=pl.Buffered(1)))
    return pl.pallas_call(
        functools.partial(head_kernel, vocab, n_chunks, n_rep, n_own, with_top),
        out_shape=out_shape,
        grid_spec=pltpu.PrefetchScalarGridSpec(
            num_scalar_prefetch=1, grid=(n_tiles,),
            in_specs=[pl.BlockSpec((n_tok, d_model), lambda j, b: (0, 0)),
                      pl.BlockSpec((2, n_tok), lambda j, b: (0, 0)),
                      pl.BlockSpec((1, n_tok), lambda j, b: (0, 0)),
                      pl.BlockSpec((TILE, d_model), lambda j, b: (jnp.minimum(tile_of(n_own, b, j), last), 0)),
                      pl.BlockSpec((TILE, d_model), lambda j, b: (jnp.minimum(b[0] + jnp.minimum(j, n_own - 1), last), 0))],
            out_specs=out_specs,
            scratch_shapes=[pltpu.VMEM((n_chunks, d_model, CHUNK), jnp.float32)] * with_top + [pltpu.VMEM((TILE, d_model), jnp.float32)]),
        compiler_params=params(),
        cost_estimate=pl.CostEstimate(flops=(6 if with_top else 4) * n_tiles * TILE * n_tok * d_model,
                                      bytes_accessed=n_tiles * TILE * d_model * 12, transcendentals=0),
        name='head_grads' if with_top else 'head_rows',
    )(blocks, z_all, norm, targets, embed_table, grad_embed)


def sparse_rows(block, start_ref, ids_ref, low_ref, base):
    rows = block * TILE + lax.broadcasted_iota(jnp.int32, (TILE, 1), 0)
    first = start_ref[block] // SEG
    stop = (start_ref[block + 1] + SEG - 1) // SEG

    def segment(c, acc):
        pick = jnp.where(rows == ids_ref[pl.ds(c, 1), :], 1.0, 0.0).astype(jnp.bfloat16)
        return acc + jnp.dot(pick, low_ref[pl.ds(pl.multiple_of(c * SEG, SEG), SEG), :], preferred_element_type=jnp.float32)

    return lax.fori_loop(first, stop, segment, base)


def sumsq_kernel(low_scale, blk_ref, start_ref, ids_ref, low_ref, g_ref, out_ref):
    block = blk_ref[0] + pl.program_id(0)
    zero = jnp.zeros(g_ref.shape, jnp.float32)
    full = g_ref[...] + low_scale * sparse_rows(block, start_ref, ids_ref, low_ref, zero)

    @pl.when(pl.program_id(0) == 0)
    def _():
        out_ref[...] = jnp.zeros_like(out_ref)

    out_ref[...] += jnp.sum((full * full).reshape(-1, 8, full.shape[1]), axis=0)


def rows_sumsq(blocks, starts, ids, low, g_rows, n_tiles, low_scale):
    d_model = g_rows.shape[1]
    return pl.pallas_call(
        functools.partial(sumsq_kernel, low_scale),
        out_shape=jax.ShapeDtypeStruct((8, d_model), jnp.float32),
        grid_spec=pltpu.PrefetchScalarGridSpec(
            num_scalar_prefetch=2, grid=(n_tiles,),
            in_specs=[pl.BlockSpec(ids.shape, lambda j, b, s: (0, 0)),
                      pl.BlockSpec(low.shape, lambda j, b, s: (0, 0)),
                      pl.BlockSpec((TILE, d_model), lambda j, b, s: (b[1] + j, 0))],
            out_specs=pl.BlockSpec((8, d_model), lambda j, b, s: (0, 0))),
        compiler_params=params(),
        name='rows_sumsq',
    )(blocks, starts, ids, low, g_rows)


def adam_kernel(low_scale, first_block, n_red, start_ref, stage_ref, clip_ref, ids_ref, low_ref, *refs):
    g_refs = refs[:1 if n_red is None else 2]
    w_ref, m_ref, v_ref = refs[len(g_refs):len(g_refs) + 3]
    w_out, m_out, v_out, acc_ref = refs[-4:]
    j = first_block + pl.program_id(0)
    rows = j * ADAM_TILE + lax.broadcasted_iota(jnp.int32, (ADAM_TILE, 1), 0)
    per = ADAM_TILE // TILE
    first = jnp.minimum(start_ref[per * j] // SEG, ids_ref.shape[0] - 1)

    def segment(c):
        pick = jnp.where(rows == ids_ref[pl.ds(c, 1), :], 1.0, 0.0).astype(jnp.bfloat16)
        return low_scale * jnp.dot(pick, low_ref[pl.ds(pl.multiple_of(c * SEG, SEG), SEG), :], preferred_element_type=jnp.float32)

    if n_red is None:
        acc_ref[...] = g_refs[0][...] + segment(first)
    else:
        is_own = pl.program_id(0) // n_red == stage_ref[0]

        @pl.when(is_own)
        def _():
            acc_ref[...] = g_refs[0][...] + segment(first)

        @pl.when(jnp.logical_not(is_own))
        def _():
            acc_ref[...] = g_refs[1][...] + segment(first)

    def add(c, _):
        acc_ref[...] += segment(c)
        return 0

    lax.fori_loop(first + 1, (start_ref[per * j + per] + SEG - 1) // SEG, add, 0)

    def part(i, _):
        r = pl.ds(pl.multiple_of(i * 32, 32), 32)
        w_new, m_new, v_new = adamw_update(w_ref[r, :], m_ref[r, :], v_ref[r, :], acc_ref[r, :], clip_ref[0])
        w_out[r, :] = w_new
        m_out[r, :] = m_new
        v_out[r, :] = v_new
        return 0

    lax.fori_loop(0, ADAM_TILE // 32, part, 0)


def embed_adam(first_block, n_blocks, grads, starts, stage, clip, ids, low, embed_table, mom, vel, low_scale, held=()):
    vocab, d_model = embed_table.shape
    n_red = n_blocks // 2 if len(grads) == 2 else None
    spec = pl.BlockSpec((ADAM_TILE, d_model), lambda j, s, t, c: (first_block + j, 0))
    shape = jax.ShapeDtypeStruct((vocab, d_model), jnp.float32)

    def half(first):
        return pl.BlockSpec((ADAM_TILE, d_model), lambda j, s, t, c: (jnp.clip(j - n_red * first(t[0]), 0, n_red - 1), 0))

    g_specs = [half(lambda t: t), half(lambda t: 1 - t)] if n_red else [pl.BlockSpec((ADAM_TILE, d_model), lambda j, s, t, c: (j, 0))]
    return pl.pallas_call(
        functools.partial(adam_kernel, low_scale, first_block, n_red),
        out_shape=[shape] * 3,
        grid_spec=pltpu.PrefetchScalarGridSpec(
            num_scalar_prefetch=3, grid=(n_blocks,),
            in_specs=[pl.BlockSpec(ids.shape, lambda j, s, t, c: (0, 0)),
                      pl.BlockSpec(low.shape, lambda j, s, t, c: (0, 0))] + g_specs + [spec] * 3 + [pl.BlockSpec(memory_space=pl.ANY)] * len(held),
            out_specs=[spec] * 3,
            scratch_shapes=[pltpu.VMEM((ADAM_TILE, d_model), jnp.float32)]),
        input_output_aliases={8 + len(grads) + i: i for i in range(len(held))},
        compiler_params=params(),
        cost_estimate=pl.CostEstimate(flops=20 * n_blocks * ADAM_TILE * d_model, bytes_accessed=28 * n_blocks * ADAM_TILE * d_model,
                                      transcendentals=0),
        name='embed_adam',
    )(starts, stage, clip, ids, low, *grads, embed_table, mom, vel, *held)


def next_kernel(scale, n_blocks, ids_ref, table_ref, wi0_ref, wo0_ref, wi1_ref, wo1_ref, out_ref, rows_ref, x_ref, acc_ref, sems):
    blk = pl.program_id(0)
    slot = lax.rem(blk, 2)
    n_ff = wi0_ref.shape[1] // FWD_CHUNK
    per = TOKEN_BLOCK // (2 * n_ff)

    def fetch(base, to_slot, first, count):
        for t in range(count):
            row = ids_ref[base + first + t]
            pltpu.make_async_copy(table_ref.at[pl.ds(row, 1), :], rows_ref.at[to_slot, pl.ds(first + t, 1), :], sems.at[to_slot]).start()

    @pl.when(blk == 0)
    def _():
        def step(i, _):
            fetch(0, 0, i * 16, 16)
            return 0
        lax.fori_loop(0, TOKEN_BLOCK // 16, step, 0)

    pltpu.make_async_copy(rows_ref.at[1 - slot], rows_ref.at[slot], sems.at[slot]).wait()
    base = jnp.minimum(blk + 1, n_blocks - 1) * TOKEN_BLOCK
    x_ref[...] = (scale * rows_ref[slot].astype(jnp.bfloat16).astype(jnp.float32)).astype(jnp.bfloat16)

    for layer, (wi_ref, wo_ref) in enumerate(((wi0_ref, wo0_ref), (wi1_ref, wo1_ref))):
        acc_ref[...] = x_ref[...].astype(jnp.float32)
        for c in range(n_ff):
            fetch(base, 1 - slot, (layer * n_ff + c) * per, per)
            cols = pl.ds(c * FWD_CHUNK, FWD_CHUNK)
            pre_act = jnp.dot(x_ref[...], wi_ref[:, cols], preferred_element_type=jnp.float32)
            bend = jnp.tanh(pre_act * (GELU_K + (GELU_K * GELU_A) * (pre_act * pre_act)))
            hidden = ((0.5 * pre_act) * (1.0 + bend)).astype(jnp.bfloat16)
            acc_ref[...] += jnp.dot(hidden, wo_ref[cols, :], preferred_element_type=jnp.float32)
        if layer == 0:
            x_ref[...] = acc_ref[...].astype(jnp.bfloat16)
        else:
            out_ref[...] = acc_ref[...].astype(jnp.bfloat16)

    @pl.when(blk == n_blocks - 1)
    def _():
        pltpu.make_async_copy(rows_ref.at[slot], rows_ref.at[1 - slot], sems.at[1 - slot]).wait()


def next_forward(ids, table, wi0, wo0, wi1, wo1, scale):
    n_tok = ids.shape[0]
    d_model = table.shape[1]
    whole = [pl.BlockSpec(w.shape, lambda j, s: (0, 0)) for w in (wi0, wo0, wi1, wo1)]
    return pl.pallas_call(
        functools.partial(next_kernel, scale, n_tok // TOKEN_BLOCK),
        out_shape=jax.ShapeDtypeStruct((n_tok, d_model), jnp.bfloat16),
        grid_spec=pltpu.PrefetchScalarGridSpec(
            num_scalar_prefetch=1, grid=(n_tok // TOKEN_BLOCK,),
            in_specs=[pl.BlockSpec(memory_space=pl.ANY)] + whole,
            out_specs=pl.BlockSpec((TOKEN_BLOCK, d_model), lambda j, s: (j, 0)),
            scratch_shapes=[pltpu.VMEM((2, TOKEN_BLOCK, d_model), jnp.float32), pltpu.VMEM((TOKEN_BLOCK, d_model), jnp.bfloat16),
                            pltpu.VMEM((TOKEN_BLOCK, d_model), jnp.float32), pltpu.SemaphoreType.DMA((2,))]),
        compiler_params=params(),
        cost_estimate=pl.CostEstimate(flops=8 * n_tok * d_model * wi0.shape[1], bytes_accessed=6 * n_tok * d_model, transcendentals=0),
        name='next_forward',
    )(ids, table, wi0, wo0, wi1, wo1)


def exchange(x_ref, all_ref, send_sems, recv_sems):
    n_stage = lax.axis_size('stage')
    me = lax.axis_index('data') * n_stage + lax.axis_index('stage')

    def place(k):
        to = lax.rem(me + k, N_DEV)
        return to // n_stage, lax.rem(to, n_stage)

    barrier = pltpu.get_barrier_semaphore()
    for k in range(1, N_DEV):
        pl.semaphore_signal(barrier, inc=1, device_id=place(k), device_id_type=MESH_ID)
    pl.semaphore_wait(barrier, N_DEV - 1)
    copies = []
    for k in range(1, N_DEV):
        copies.append(pltpu.make_async_remote_copy(
            src_ref=x_ref, dst_ref=all_ref.at[k - 1], send_sem=send_sems.at[k - 1], recv_sem=recv_sems.at[k - 1],
            device_id=place(k), device_id_type=MESH_ID))
        copies[-1].start()
    for copy in copies:
        copy.wait()


def norm_kernel(x_ref, out_ref, all_ref, send_sems, recv_sems):
    exchange(x_ref, all_ref, send_sems, recv_sems)
    top = x_ref[0:1, :]
    for k in range(N_DEV - 1):
        top = jnp.maximum(top, all_ref[k, 0:1, :])
    total = x_ref[1:2, :] * jnp.exp(x_ref[0:1, :] - top)
    for k in range(N_DEV - 1):
        total += all_ref[k, 1:2, :] * jnp.exp(all_ref[k, 0:1, :] - top)
    out_ref[0:1, :] = top
    out_ref[1:2, :] = 1.0 / total


def gather_kernel(x_ref, out_ref, all_ref, send_sems, recv_sems):
    exchange(x_ref, all_ref, send_sems, recv_sems)
    me = lax.axis_index('data') * lax.axis_size('stage') + lax.axis_index('stage')
    out_ref[pl.ds(me, 1)] = x_ref[...][None]
    for k in range(N_DEV - 1):
        out_ref[pl.ds(lax.rem(me + (N_DEV - 1 - k), N_DEV), 1)] = all_ref[k:k + 1]


def small_exchange(body, x, out_shape, collective_id, name):
    return pl.pallas_call(
        body,
        out_shape=out_shape,
        in_specs=[pl.BlockSpec(memory_space=pltpu.VMEM)],
        out_specs=pl.BlockSpec(memory_space=pltpu.VMEM),
        scratch_shapes=[pltpu.VMEM((N_DEV - 1,) + x.shape, x.dtype), pltpu.SemaphoreType.DMA((N_DEV - 1,)),
                        pltpu.SemaphoreType.DMA((N_DEV - 1,))],
        compiler_params=pltpu.CompilerParams(collective_id=collective_id, has_side_effects=True),
        name=name,
    )(x)


def solution(mesh):
    n_stage = mesh.shape['stage']
    n_rep = mesh.shape['data']
    n_dev = n_stage * n_rep
    swap = [(0, 1), (1, 0)]
    w_spec = P('stage', None, None)
    in_specs = (w_spec,) * 8 + (P(None, None),) * 4 + (P('stage', 'data', None), P('data'), P('data'), P(None, 'data'), P(None))
    out_specs = (w_spec,) * 6 + (P(None, None),) * 3 + (P(None, 'data', None),)

    def local_step(w_first, w_second, mom_first, mom_second, vel_first, vel_second, grad_first, grad_second,
                   embed_table, mom_embed, vel_embed, grad_embed, stage_acts, last_tokens, targets, next_tokens, max_norm):
        stage_id = lax.axis_index('stage')
        dev_id = lax.axis_index('data') * n_stage + stage_id
        low_core = stage_id == 0
        vocab, d_model = embed_table.shape
        scale_in = math.sqrt(d_model)
        low_scale = scale_in / n_rep
        n_tiles = -(-vocab // (TILE * n_dev))
        n_wide = WIDE_TILES
        n_rest = n_tiles - n_wide
        n_red = n_rest * n_dev // n_stage
        n_part = n_red // n_rep
        rest0 = n_dev * n_wide

        def other(x):
            return lax.ppermute(x, 'stage', swap)

        def by_stage(own, far):
            return jnp.where(low_core, own, far), jnp.where(low_core, far, own)

        w_in, w_out = w_first[0].astype(jnp.bfloat16), w_second[0].astype(jnp.bfloat16)
        w_in0, w_in1 = by_stage(w_in, other(w_in))
        w_out0, w_out1 = by_stage(w_out, other(w_out))

        z_own = block_forward(stage_acts[0], w_in, w_out)
        cut = z_own.shape[0] // 2
        z_piece = jnp.where(low_core, lax.ppermute(z_own[:cut], 'stage', [(1, 0)]), z_own[cut:])
        all_ids = lax.all_gather(jnp.stack([last_tokens, targets]), 'data', axis=1, tiled=True)
        ids, tgts = all_ids[0], all_ids[1:2]
        n_tok = ids.shape[0]
        half = n_tok // 2
        z_all = lax.all_gather(z_piece, BOTH, axis=0, tiled=True)

        order = jnp.arange(n_tok, dtype=jnp.int32)
        before = (ids[None, :] < ids[:, None]) | ((ids[None, :] == ids[:, None]) & (order[None, :] < order[:, None]))
        rank = jnp.sum(before.astype(jnp.int32), axis=1)
        edges = TILE * jnp.arange(n_tiles * n_dev + 1, dtype=jnp.int32)
        starts = jnp.sum((ids[None, :] < edges[:, None]).astype(jnp.int32), axis=1)
        z_all, rank, starts, acts_in = lax.optimization_barrier((z_all, rank, starts, stage_acts[0]))

        acts = lax.all_gather(acts_in, 'data', axis=0, tiled=True)

        def blocks(*tiles):
            return jnp.stack([jnp.asarray(t, jnp.int32) for t in tiles])

        shard = blocks(dev_id * n_wide, rest0 + dev_id * n_rest - n_wide)
        stat = head_stats(z_all, embed_table, shard, n_wide, n_tiles)
        norm = small_exchange(norm_kernel, stat, jax.ShapeDtypeStruct(stat.shape, jnp.float32), 1, 'share_stats')
        norm, acts = lax.optimization_barrier((norm, acts))
        mine = lax.dynamic_slice_in_dim(acts, stage_id * half, half)
        far = other(lax.dynamic_slice_in_dim(acts, (1 - stage_id) * half, half))
        act0, act1 = by_stage(mine, far)
        g_shard, d_top_part = head_grads(z_all, norm, tgts, embed_table, grad_embed, shard, n_wide, n_tiles, n_rep, True)
        d_top_own = lax.psum_scatter(d_top_part, BOTH, scatter_dimension=0, tiled=True)
        red_tile = rest0 + stage_id * n_red
        red = blocks(red_tile, red_tile)
        n_early = n_red - n_red // 4
        g_own = head_rows(z_all, norm, tgts, embed_table, grad_embed, red, n_red, 0, n_early, n_rep)
        d_top_own, g_own = lax.optimization_barrier((d_top_own, g_own))
        d_top_own = d_top_own.reshape(-1, d_model).astype(jnp.bfloat16)
        g_shard, d_top_own, late_ids = lax.optimization_barrier((g_shard, d_top_own, ids))
        d_top = lax.all_gather(d_top_own, BOTH, axis=0, tiled=True)
        sorted_ids = jnp.sum(jnp.where(rank[None, :] == order[:, None], late_ids[None, :], 0), axis=1).reshape(n_tok // SEG, SEG)
        g_own = head_rows(z_all, norm, tgts, embed_table, grad_embed, red, n_red, n_early, n_red - n_early, n_rep, g_own)
        d_top, sorted_ids, g_own = lax.optimization_barrier((d_top, sorted_ids, g_own))
        g_far = other(g_own)
        g_wide = lax.all_gather(g_shard, BOTH, axis=0, tiled=True)

        d_half = lax.dynamic_slice_in_dim(d_top, stage_id * half, half)
        olds = (grad_first[0], grad_second[0], n_rep)
        d_act1, full_in1, full_out1, sq1 = block_backward(d_half, act1, w_in1, w_out1, *olds, 3)
        d_low_half, full_in0, full_out0, sq0 = block_backward(d_act1, act0, w_in0, w_out0, *olds, 4)
        my_rank = lax.dynamic_slice_in_dim(rank, stage_id * half, half)
        perm = (my_rank[None, :] == order[:, None]).astype(jnp.bfloat16)
        low_half = jnp.dot(perm, d_low_half, preferred_element_type=jnp.float32).astype(jnp.bfloat16)
        low = low_half + other(low_half)

        full_first = jnp.where(low_core, full_in0, full_in1)
        full_second = jnp.where(low_core, full_out0, full_out1)

        my_part = lax.axis_index('data') * n_part
        embed_sq = (jnp.sum(rows_sumsq(blocks(dev_id * n_wide, 0), starts, sorted_ids, low, g_shard, n_wide, low_scale))
                    + jnp.sum(rows_sumsq(blocks(red_tile + my_part, my_part), starts, sorted_ids, low, g_own, n_part, low_scale)))
        stage_sq = jnp.sum(jnp.where(low_core, sq0, sq1))
        own_sq = jnp.full((8, 128), embed_sq + stage_sq / n_rep)
        all_sq = small_exchange(gather_kernel, own_sq, jax.ShapeDtypeStruct((n_dev, 8, 128), jnp.float32), 2, 'share_sums')
        total_sq = jnp.sum(all_sq[:, 0, 0])
        clip_scale = jnp.minimum(1.0, max_norm[0] / (jnp.sqrt(total_sq) + CLIP_EPS))
        new_first, new_mom_first, new_vel_first = adamw_update(w_first[0], mom_first[0], vel_first[0], full_first, clip_scale)
        new_second, new_mom_second, new_vel_second = adamw_update(w_second[0], mom_second[0], vel_second[0], full_second, clip_scale)
        n_first = rest0 * TILE // ADAM_TILE
        update = (starts, blocks(stage_id), clip_scale.reshape(1), sorted_ids, low, embed_table, mom_embed, vel_embed, low_scale)
        rest_rows = embed_adam(n_first, -(-vocab // ADAM_TILE) - n_first, (g_own, g_far), *update)
        new_embed, new_mom_embed, new_vel_embed = embed_adam(0, n_first, (g_wide,), *update, held=tuple(rest_rows))

        next_in, next_out = new_first.astype(jnp.bfloat16), new_second.astype(jnp.bfloat16)
        next_in0, next_in1 = by_stage(next_in, other(next_in))
        next_out0, next_out1 = by_stage(next_out, other(next_out))
        n_micro, tokens = next_tokens.shape
        my_micro = n_micro // n_stage
        my_rows = lax.dynamic_slice_in_dim(next_tokens, stage_id * my_micro, my_micro).reshape(2, -1)
        gathered = []
        for piece in range(2):
            final_act = next_forward(my_rows[piece], new_embed, next_in0, next_out0, next_in1, next_out1, scale_in)
            gathered.append(lax.all_gather(final_act.reshape(my_micro // 2, tokens, d_model), 'stage', axis=0, tiled=False))
        next_acts = jnp.stack(gathered, axis=1).reshape(n_micro, tokens, d_model)
        return (new_first[None], new_second[None], new_mom_first[None], new_mom_second[None],
                new_vel_first[None], new_vel_second[None], new_embed, new_mom_embed, new_vel_embed, next_acts)

    return jax.shard_map(local_step, mesh=mesh, in_specs=in_specs, out_specs=out_specs, check_vma=False)
```
